128 devices in a mesh: rows: 16 (over z_hi, x, core), cols: 8 (over z_lo, y).
Axes of the slice: x: 4, y: 4, z: 4 (z_hi: 2, z_lo: 2; z = z_hi * 2 + z_lo), core: 2. Of those that a mesh axis runs over, the one named last changes fastest.
Arguments:
- surface_field: float32 [8192, 16384], P('rows', 'cols'), may hold values from -20 to 30
- land_words: int32 [8192, 512], P('rows', 'cols'), may hold values from -2147483648 to 2147483646
Outputs:
- level_one: float32 [4096, 8192], P('rows', 'cols')
- level_two: float32 [2048, 4096], P('rows', 'cols')
- level_three: float32 [1024, 2048], P('rows', 'cols')
- level_four: float32 [512, 1024], P('rows', 'cols')
- level_means: float32 [4], replicated
- level_maxima: float32 [4], replicated
The draws below stay inside these ranges and needn't reach their ends.
All inputs are finite; a program needn't handle non-finite values.
Results may differ from the reference program's by a relative error of at most 0.0001.
Values sent between devices are 32-bit elements; how exact they have to be, the bound alone decides.
A program may use at most 128 MiB of HBM per device.

```python
import math
import jax
import jax.numpy as jnp

NY = 8192
NX = 16384


def draw_surface_field(key, part):
    noise_key = jax.random.fold_in(jax.random.fold_in(key, 11), 0)
    rows_frac = jnp.arange(NY, dtype=jnp.float32) / NY
    cols_frac = jnp.arange(NX, dtype=jnp.float32) / NX
    trend = (1.0 + 2.0 * rows_frac)[:, None] * (1.0 + 2.0 * cols_frac)[None, :]
    noise = jnp.clip(jax.random.normal(noise_key, (NY, NX), jnp.float32), -6.0, 6.0)
    return (trend + noise).astype(jnp.float32)


def touch_ends(values, key, smallest, top_value):
    index_at = [jax.random.randint(jax.random.fold_in(key, axis), (), 0, length) for axis, length in enumerate(values.shape)]
    main_axis = values.shape.index(max(values.shape))
    next_to = index_at[:main_axis] + [(index_at[main_axis] + 1) % values.shape[main_axis]] + index_at[main_axis + 1:]
    return values.at[tuple(index_at)].set(smallest).at[tuple(next_to)].set(top_value)


def setup_inputs(seed: int = 0) -> dict:
    splits = jax.random.split(jax.random.key(seed), 3)
    surface_field = draw_surface_field(jax.random.fold_in(splits[2], 71), 0)
    land_words = touch_ends(jax.random.randint(splits[1], (NY, NX // 32), -2147483648, 2147483647), jax.random.fold_in(splits[1], 1), -2147483648, 2147483646).astype(jnp.int32)
    return dict(surface_field=surface_field, land_words=land_words)


stencil_weights = (0.125, 0.375, 0.375, 0.125)
floor_value = 0.05
mean_eps = 1e-6


def coarsen(extended):
    count_rows = (extended.shape[1] - 2) // 2
    count_cols = (extended.shape[2] - 2) // 2
    across = stencil_weights[0] * extended[:, :, 0:2 * count_cols:2]
    for offset in range(1, 4):
        across = across + stencil_weights[offset] * extended[:, :, offset:offset + 2 * count_cols:2]
    downward = stencil_weights[0] * across[:, 0:2 * count_rows:2, :]
    for offset in range(1, 4):
        downward = downward + stencil_weights[offset] * across[:, offset:offset + 2 * count_rows:2, :]
    return downward


def finish(partial_value):
    values = partial_value[0] / jnp.maximum(partial_value[1], floor_value)
    covers = partial_value[1]
    return values, covers, jnp.stack([covers * values, covers])


def reference(surface_field, land_words):
    expanded = jnp.repeat(land_words, 32, axis=1)
    shifts = jnp.arange(expanded.shape[1], dtype=jnp.int32) % 32
    land_flag = jnp.bitwise_and(jnp.right_shift(expanded, shifts[None, :]), 1)
    rows_index = jnp.arange(NY, dtype=jnp.int32).astype(jnp.float32)
    latitude = ((rows_index + 0.5) / NY - 0.5) * math.pi
    covers = land_flag.astype(jnp.float32) * jnp.cos(latitude)[:, None]
    stacked = jnp.stack([covers * surface_field, covers])
    outputs = []
    weighted = []
    totals = []
    maxima = []
    for level_step in range(4):
        wrapped = jnp.concatenate([stacked[:, :, -1:], stacked, stacked[:, :, :1]], axis=2)
        padded = jnp.pad(wrapped, ((0, 0), (1, 1), (0, 0)))
        values, covers, stacked = finish(coarsen(padded))
        outputs.append(values)
        weighted.append(jnp.sum(stacked[0]))
        totals.append(jnp.sum(covers))
        maxima.append(jnp.max(values))
    level_means = jnp.stack(weighted) / (jnp.stack(totals) + mean_eps)
    return outputs[0], outputs[1], outputs[2], outputs[3], level_means, jnp.stack(maxima)
```

```python
import math

import jax
import jax.numpy as jnp
from jax import lax
from jax.experimental import pallas as pl
from jax.experimental.pallas import tpu as pltpu
from jax.sharding import PartitionSpec as P

MESH = pl.DeviceIdType.MESH
F32 = jnp.float32
BF16 = jnp.bfloat16
HALO = 16
PAD = 24
LANES = 128
ROW_CHUNK = 64
FLOOR = 0.05
EPS = 1e-06


def lane_iota(rows, dtype=jnp.int32):
    return lax.broadcasted_iota(dtype, (rows, LANES), 1)


def tap_weight(offset):
    inner = jnp.logical_or(offset == 1, offset == 2)
    outer = jnp.logical_or(offset == 0, offset == 3)
    return jnp.where(inner, 0.375, jnp.where(outer, 0.125, 0.0))


def build_tables(band, edge):
    k = lax.broadcasted_iota(jnp.int32, (256, 256), 0)
    n = lax.broadcasted_iota(jnp.int32, (256, 256), 1)
    own = tap_weight(k - (2 * n - 1))
    spill = jnp.logical_or(
        jnp.logical_and(n == 128, k == 255), jnp.logical_and(n == 255, k == 0)
    )
    table = jnp.where(n < 128, own, jnp.where(spill, 0.125, 0.0)).astype(BF16)
    band[0:256, :] = table
    band[256:512, :] = table
    k = lax.broadcasted_iota(jnp.int32, (128, 256), 0)
    n = lax.broadcasted_iota(jnp.int32, (128, 256), 1)
    right = jnp.where(k < 64, tap_weight(k - (2 * n - 1)), 0.0)
    left = jnp.where(k >= 64, tap_weight(k - (2 * n - 129)), 0.0)
    spill = jnp.logical_or(
        jnp.logical_and(n == 128, k == 127), jnp.logical_and(n == 255, k == 0)
    )
    table = jnp.where(
        n < 64, right, jnp.where(n < 128, left, jnp.where(spill, 0.125, 0.0))
    ).astype(BF16)
    edge[0:128, :] = table
    edge[128:256, :] = table


def pieces(x):
    high = x.astype(BF16)
    low = (x - high.astype(F32)).astype(BF16)
    return high, low


def land_of(words, tile):
    rows = words.shape[0]
    lane = lane_iota(rows)
    picked = jnp.take_along_axis(
        words, 4 * tile + lane // 32, axis=1, mode="promise_in_bounds"
    )
    return jnp.left_shift(picked, 31 - lane % 32) < 0


def wide(words):
    if words.shape[1] < LANES:
        words = jnp.concatenate([words] * (LANES // words.shape[1]), axis=1)
    return words


def dot(a, b):
    return jnp.dot(a, b, preferred_element_type=F32)


def first_across(field_tile, words, rows, s_num, s_den, r_num, r_den, band, tiles, store):
    words = wide(words)
    for tile in range(tiles):
        land = land_of(words, tile)
        masked = jnp.where(land, field_tile(tile), 0.0)
        high, low = pieces(masked)
        at = (tile // 2) * rows
        half = (tile % 2) * LANES
        s_num[at : at + rows, half : half + LANES] = high
        s_num[at : at + rows, 256 + half : 256 + half + LANES] = low
        s_den[at : at + rows, half : half + LANES] = jnp.where(land, 1.0, 0.0).astype(BF16)
    blocks = tiles // 2
    r_num[0 : blocks * rows, :] = dot(s_num[0 : blocks * rows, :], band[...])
    r_den[0 : blocks * rows, :] = dot(s_den[0 : blocks * rows, :], band[0:256, :])
    low_half = lane_iota(rows) < 64
    for which, ref in ((0, r_num), (1, r_den)):
        def spill(block):
            if block < 0 or block >= blocks:
                return jnp.zeros((rows, LANES), F32)
            return ref[block * rows : (block + 1) * rows, LANES : 2 * LANES]

        for block in range(blocks):
            own = ref[block * rows : (block + 1) * rows, 0:LANES]
            store(which, block, own + jnp.where(low_half, spill(block - 1), spill(block + 1)))
        store(which, blocks, jnp.where(low_half, spill(blocks - 1), spill(0)))


def kernel(
    field_hbm, words_hbm,
    v1, v2, v3, v4, stats,
    fld, wrd, fhal, whal, out_left, out_right, in_left, in_right, cornf, cornw,
    s_num, s_den, r_num, r_den, se_num, se_den, re_num, re_den,
    hn, hd, cosb, p1, d1, p2, d2, p3, d3,
    sx, sxe, rx, rxe, band, edge, msg_a, msg_b, slot_a, slot_b,
    load_sem, send_sem, recv_sem, a_send, a_recv, b_send, b_recv,
):
    n_rows, n_cols = lax.axis_size("rows"), lax.axis_size("cols")
    my_row, my_col = lax.axis_index("rows"), lax.axis_index("cols")
    rows, cols = fld.shape
    tiles = cols // LANES
    up, down = lax.rem(my_row + n_rows - 1, n_rows), lax.rem(my_row + 1, n_rows)
    left, right = lax.rem(my_col + n_cols - 1, n_cols), lax.rem(my_col + 1, n_cols)

    barrier = pltpu.get_barrier_semaphore()
    peers = [(my_row, lax.rem(my_col + s, n_cols)) for s in range(1, n_cols)]
    peers += [(lax.rem(my_row + s, n_rows), my_col) for s in range(1, n_rows)]
    peers += [(up, left), (up, right), (down, left), (down, right)]
    for peer in peers:
        pl.semaphore_signal(barrier, inc=1, device_id=peer, device_id_type=MESH)

    loads = []

    def load(src, dst):
        copy = pltpu.make_async_copy(src, dst, load_sem.at[len(loads)])
        copy.start()
        loads.append(copy)
        return copy

    load_words = load(words_hbm, wrd)
    load_strips = [
        load(field_hbm.at[:, 0:LANES], fld.at[:, 0:LANES]),
        load(field_hbm.at[:, cols - LANES : cols], fld.at[:, cols - LANES : cols]),
    ]
    chunks = rows // ROW_CHUNK
    order = [0, chunks - 1] + list(range(1, chunks - 1))
    load_chunk = {}
    for c in order:
        at = pl.ds(c * ROW_CHUNK, ROW_CHUNK)
        load_chunk[c] = load(
            field_hbm.at[at, LANES : cols - LANES], fld.at[at, LANES : cols - LANES]
        )

    build_tables(band, edge)
    for ref in (hn, hd, p1, d1, p2, d2, p3, d3):
        spare = PAD - HALO if ref.shape[1] == rows + 2 * PAD else HALO
        zeros = jnp.zeros((ref.shape[0], spare, LANES), F32)
        ref[:, 0:spare, :] = zeros
        ref[:, ref.shape[1] - spare :, :] = zeros

    sub = lax.broadcasted_iota(jnp.int32, (8, LANES), 0)
    global_row = my_row * rows - PAD + sub * LANES + lane_iota(8)
    latitude = ((global_row.astype(F32) + 0.5) / (rows * n_rows) - 0.5) * math.pi
    cosines = jnp.cos(latitude) * 0.125
    for q in range(cosb.shape[0] // LANES):
        row = jnp.broadcast_to(cosines[q : q + 1, :], (LANES, LANES))
        cosb[q * LANES : (q + 1) * LANES, :] = jnp.transpose(row)

    load_words.wait()
    for copy in load_strips:
        copy.wait()
    packed = rows // 8
    lane = lane_iota(packed)
    for out, tile, shift in ((out_left, 0, 0), (out_right, tiles - 1, HALO)):
        field_part = jnp.zeros((packed, LANES), F32)
        land_part = jnp.zeros((packed, LANES), F32)
        for g in range(8):
            at = slice(g * packed, (g + 1) * packed)
            values = fld[at, tile * LANES : (tile + 1) * LANES]
            land = jnp.where(land_of(wide(wrd[at, :]), tile), 1.0, 0.0)
            turn = (HALO * g + shift) % LANES
            if turn:
                values, land = pltpu.roll(values, turn, 1), pltpu.roll(land, turn, 1)
            here = lane // HALO == g
            field_part = jnp.where(here, values, field_part)
            land_part = jnp.where(here, land, land_part)
        out[0:packed, :] = field_part
        out[packed : 2 * packed, :] = land_part
    load_chunk[0].wait()
    if chunks > 1:
        load_chunk[chunks - 1].wait()

    pl.semaphore_wait(barrier, len(peers))

    sends = []

    def send(src, dst, row, col):
        i = len(sends)
        copy = pltpu.make_async_remote_copy(
            src_ref=src, dst_ref=dst, send_sem=send_sem.at[i], recv_sem=recv_sem.at[i],
            device_id=(row, col), device_id_type=MESH,
        )
        copy.start()
        sends.append(copy)

    top, bottom = slice(0, HALO), slice(rows - HALO, rows)
    last_tile = slice(cols - LANES, cols)
    send(out_left, in_right, my_row, left)
    send(out_right, in_left, my_row, right)
    send(fld.at[top, :], fhal.at[HALO : 2 * HALO, :], up, my_col)
    send(fld.at[bottom, :], fhal.at[0:HALO, :], down, my_col)
    send(wrd.at[top, :], whal.at[HALO : 2 * HALO, :], up, my_col)
    send(wrd.at[bottom, :], whal.at[0:HALO, :], down, my_col)
    send(fld.at[bottom, last_tile], cornf.at[0 * HALO : 1 * HALO, :], down, right)
    send(fld.at[bottom, 0:LANES], cornf.at[1 * HALO : 2 * HALO, :], down, left)
    send(fld.at[top, last_tile], cornf.at[2 * HALO : 3 * HALO, :], up, right)
    send(fld.at[top, 0:LANES], cornf.at[3 * HALO : 4 * HALO, :], up, left)
    send(wrd.at[bottom, :], cornw.at[0 * HALO : 1 * HALO, :], down, right)
    send(wrd.at[bottom, :], cornw.at[1 * HALO : 2 * HALO, :], down, left)
    send(wrd.at[top, :], cornw.at[2 * HALO : 3 * HALO, :], up, right)
    send(wrd.at[top, :], cornw.at[3 * HALO : 4 * HALO, :], up, left)

    for c in order[2:]:
        load_chunk[c].wait()

    def own_rows(c, carry):
        at = pl.multiple_of(c * ROW_CHUNK, ROW_CHUNK)

        def field_tile(tile):
            return fld[pl.ds(at, ROW_CHUNK), tile * LANES : (tile + 1) * LANES]

        def store(which, tile, value):
            ref = (hn, hd)[which]
            ref[tile, pl.ds(PAD + at, ROW_CHUNK), :] = value

        first_across(
            field_tile, wrd[pl.ds(at, ROW_CHUNK), :], ROW_CHUNK,
            s_num, s_den, r_num, r_den, band, tiles, store,
        )
        return carry

    lax.fori_loop(0, chunks, own_rows, 0)

    for copy in sends:
        copy.wait()

    def halo_store(which, tile, value):
        ref = (hn, hd)[which]
        ref[tile, PAD - HALO : PAD, :] = value[0:HALO, :]
        ref[tile, PAD + rows : PAD + rows + HALO, :] = value[HALO : 2 * HALO, :]

    first_across(
        lambda tile: fhal[:, tile * LANES : (tile + 1) * LANES], whal[...], 2 * HALO,
        s_num, s_den, r_num, r_den, band, tiles, halo_store,
    )

    def edge_store(at, count, field_value, land_value):
        high, low = pieces(field_value * land_value)
        se_num[at : at + count, 0:LANES] = high
        se_num[at : at + count, LANES : 2 * LANES] = low
        se_den[at : at + count, :] = land_value.astype(BF16)

    for g in range(8):
        parts = []
        for base in (0, packed):
            from_right = in_right[base : base + packed, :]
            from_left = in_left[base : base + packed, :]
            turn = (LANES - HALO * g) % LANES
            if turn:
                from_right = pltpu.roll(from_right, turn, 1)
            turn = (LANES - HALO - HALO * g) % LANES
            if turn:
                from_left = pltpu.roll(from_left, turn, 1)
            parts.append(
                jnp.where(
                    lane < HALO, from_right, jnp.where(lane >= LANES - HALO, from_left, 0.0)
                )
            )
        edge_store(g * packed, packed, parts[0], parts[1])
    lane16 = lane_iota(HALO)
    for side in range(2):
        l_at = slice(2 * side * HALO, (2 * side + 1) * HALO)
        r_at = slice((2 * side + 1) * HALO, (2 * side + 2) * HALO)
        is_right, is_left = lane16 < HALO, lane16 >= LANES - HALO
        value = jnp.where(is_right, cornf[r_at, :], jnp.where(is_left, cornf[l_at, :], 0.0))
        land_r = jnp.where(land_of(wide(cornw[r_at, :]), 0), 1.0, 0.0)
        land_l = jnp.where(land_of(wide(cornw[l_at, :]), tiles - 1), 1.0, 0.0)
        land = jnp.where(is_right, land_r, jnp.where(is_left, land_l, 0.0))
        edge_store(rows + side * HALO, HALO, value, land)
    re_num[...] = dot(se_num[...], edge[...])
    re_den[...] = dot(se_den[...], edge[0:128, :])
    out_tiles = tiles // 2

    def merge_edge(src, dst, count):
        low_half = lane_iota(count) < 64
        for result, ref in ((re_num, hn), (re_den, hd)):
            spill = result[pl.ds(src, count), LANES : 2 * LANES]
            here = pl.ds(dst, count)
            last = out_tiles - 1
            ref[0, here, :] = ref[0, here, :] + jnp.where(low_half, spill, 0.0)
            ref[last, here, :] = ref[last, here, :] + jnp.where(low_half, 0.0, spill)
            ref[out_tiles, here, :] = ref[out_tiles, here, :] + result[pl.ds(src, count), 0:LANES]

    def merge_own(c, carry):
        at = pl.multiple_of(c * ROW_CHUNK, ROW_CHUNK)
        merge_edge(at, PAD + at, ROW_CHUNK)
        return carry

    lax.fori_loop(0, chunks, merge_own, 0)
    merge_edge(rows, PAD - HALO, HALO)
    merge_edge(rows + HALO, PAD + rows, HALO)

    inside_top, inside_bottom = my_row > 0, my_row < n_rows - 1
    out_rows = rows // 2

    def finish(num, den):
        value = num / jnp.maximum(den, FLOOR)
        return value, den * value

    def level_one_rows(i0, tile, cosine):
        result = []
        for ref in (hn, hd):
            taps = [ref[tile, pl.ds(PAD + 2 * i0 - 1 + a, 8, stride=2), :] for a in range(4)]
            taps = [t * c for t, c in zip(taps, cosine)]
            result.append((taps[0] + taps[3]) + (taps[1] + taps[2]))
        return result

    def cosine_of(i0):
        taps = [cosb[pl.ds(PAD + 2 * i0 - 1 + a, 8, stride=2), :] for a in range(4)]
        return [taps[0], 3.0 * taps[1], 3.0 * taps[2], taps[3]]

    zero_sums = (
        jnp.zeros((8, LANES), F32), jnp.zeros((8, LANES), F32), jnp.full((8, LANES), -jnp.inf, F32)
    )

    def gather_sums(sums, value, product, cover):
        return (sums[0] + product, sums[1] + cover, jnp.maximum(sums[2], value))

    def level_one(c, sums):
        i0 = pl.multiple_of(c * 8, 8)
        cosine = cosine_of(i0)
        for tile in range(out_tiles + 1):
            at = slice(tile * LANES, (tile + 1) * LANES)
            num, den = level_one_rows(i0, tile, cosine)
            value, product = finish(num, den)
            p1[tile, pl.ds(PAD + i0, 8), :] = product
            d1[tile, pl.ds(PAD + i0, 8), :] = den
            if tile < out_tiles:
                v1[pl.ds(i0, 8), at] = value
                sums = gather_sums(sums, value, product, den)
        return sums

    all_sums = [lax.fori_loop(0, out_rows // 8, level_one, zero_sums)]
    for i0, keep in ((-8, inside_top), (out_rows, inside_bottom)):
        cosine = cosine_of(i0)
        for tile in range(out_tiles + 1):
            num, den = level_one_rows(i0, tile, cosine)
            value, product = finish(num, den)
            p1[tile, PAD + i0 : PAD + i0 + 8, :] = jnp.where(keep, product, 0.0)
            d1[tile, PAD + i0 : PAD + i0 + 8, :] = jnp.where(keep, den, 0.0)

    def next_level(pin, din, pout, dout, vout):
        out_rows, out_cols = vout.shape
        blocks = out_cols // LANES
        last_level = pout is None
        count = out_rows if last_level else out_rows + HALO

        def down_rows(ref, i0, size, tile):
            taps = [ref[tile, pl.ds(PAD + 2 * i0 - 1 + a, size, stride=2), :] for a in range(4)]
            return 0.125 * (taps[0] + taps[3]) + 0.375 * (taps[1] + taps[2])

        def put(which, tile, m0, value):
            high, low = pieces(value)
            if tile < 2 * blocks:
                base = (which * blocks + tile // 2) * count + m0
                half = (tile % 2) * LANES
                sx[pl.ds(base, 16), half : half + LANES] = high
                sx[pl.ds(base, 16), 256 + half : 256 + half + LANES] = low
            else:
                base = which * count + m0
                sxe[pl.ds(base, 16), 0:LANES] = high
                sxe[pl.ds(base, 16), LANES : 2 * LANES] = low

        def rows_step(c, carry):
            i0 = pl.multiple_of(c * 16, 16)
            for which, ref in ((0, pin), (1, din)):
                for tile in range(2 * blocks + 1):
                    value = jnp.concatenate(
                        [down_rows(ref, i0, 8, tile), down_rows(ref, i0 + 8, 8, tile)], axis=0
                    )
                    put(which, tile, i0, value)
            return carry

        lax.fori_loop(0, out_rows // 16, rows_step, 0)
        if not last_level:
            for which, ref in ((0, pin), (1, din)):
                for tile in range(2 * blocks + 1):
                    value = jnp.concatenate(
                        [down_rows(ref, -8, 8, tile), down_rows(ref, out_rows, 8, tile)], axis=0
                    )
                    put(which, tile, out_rows, value)
        total = 2 * blocks * count
        rx[0:total, :] = dot(sx[0:total, :], band[...])
        rxe[0 : 2 * count, :] = dot(sxe[0 : 2 * count, :], edge[...])
        low_half = lane_iota(8) < 64

        def across(m0, tile):
            result = []
            for which in range(2):
                def piece(block, half):
                    block = block % (blocks + 1)
                    at = slice(half * LANES, (half + 1) * LANES)
                    if block == blocks:
                        return rxe[pl.ds(which * count + m0, 8), at]
                    return rx[pl.ds((which * blocks + block) * count + m0, 8), at]

                result.append(
                    piece(tile, 0)
                    + jnp.where(low_half, piece(tile - 1, 1), piece(tile + 1, 1))
                )
            return result

        def finish_step(c, sums):
            i0 = pl.multiple_of(c * 8, 8)
            for tile in range(blocks + (0 if last_level else 1)):
                at = slice(tile * LANES, (tile + 1) * LANES)
                num, den = across(i0, tile)
                value, product = finish(num, den)
                if not last_level:
                    pout[tile, pl.ds(PAD + i0, 8), :] = product
                    dout[tile, pl.ds(PAD + i0, 8), :] = den
                if tile < blocks:
                    vout[pl.ds(i0, 8), at] = value
                    sums = gather_sums(sums, value, product, den)
            return sums

        sums = lax.fori_loop(0, out_rows // 8, finish_step, zero_sums)
        if not last_level:
            for m0, i0, keep in (
                (out_rows, -8, inside_top), (out_rows + 8, out_rows, inside_bottom)
            ):
                for tile in range(blocks + 1):
                    num, den = across(m0, tile)
                    value, product = finish(num, den)
                    pout[tile, PAD + i0 : PAD + i0 + 8, :] = jnp.where(keep, product, 0.0)
                    dout[tile, PAD + i0 : PAD + i0 + 8, :] = jnp.where(keep, den, 0.0)
        return sums

    all_sums.append(next_level(p1, d1, p2, d2, v2))
    all_sums.append(next_level(p2, d2, p3, d3, v3))
    all_sums.append(next_level(p3, d3, None, None, v4))

    lane = lane_iota(8)
    message = jnp.zeros((8, LANES), F32)

    def whole(x, op):
        return op(op(x, axis=0, keepdims=True), axis=1, keepdims=True)

    for level, sums in enumerate(all_sums):
        for place, (part, op) in enumerate(zip(sums, (jnp.sum, jnp.sum, jnp.max))):
            here = jnp.logical_and(sub == place, lane == level)
            message = jnp.where(here, whole(part, op), message)

    def exchange(message, buffer, slots, send_sems, recv_sems, index, count, device):
        buffer[...] = message
        slots[index] = message
        copies = []
        for s in range(1, count):
            peer = lax.rem(index + s, count)
            copy = pltpu.make_async_remote_copy(
                src_ref=buffer, dst_ref=slots.at[index],
                send_sem=send_sems.at[s], recv_sem=recv_sems.at[index],
                device_id=device(peer), device_id_type=MESH,
            )
            copy.start()
            copies.append(copy)
        for s in range(1, count):
            peer = lax.rem(index + s, count)
            pltpu.make_async_remote_copy(
                src_ref=buffer, dst_ref=slots.at[peer],
                send_sem=send_sems.at[s], recv_sem=recv_sems.at[peer],
                device_id=device(peer), device_id_type=MESH,
            ).wait_recv()
        added, largest = slots[0], slots[0]
        for i in range(1, count):
            added, largest = added + slots[i], jnp.maximum(largest, slots[i])
        for copy in copies:
            copy.wait_send()
        return jnp.where(sub == 2, largest, added)

    message = exchange(
        message, msg_a, slot_a, a_send, a_recv, my_col, n_cols, lambda peer: (my_row, peer)
    )
    message = exchange(
        message, msg_b, slot_b, b_send, b_recv, my_row, n_rows, lambda peer: (peer, my_col)
    )
    means = message[0:1, :] / (message[1:2, :] + EPS)
    stats[...] = jnp.where(sub == 0, means, jnp.where(sub == 1, message[2:3, :], 0.0))


def per_device(surface_field, land_words):
    rows, cols = surface_field.shape
    n_rows, n_cols = lax.axis_size("rows"), lax.axis_size("cols")
    words = land_words.shape[1]
    chunks = rows // ROW_CHUNK
    blocks = cols // 256
    packed = rows // 8

    def vmem(*shape, dtype=F32):
        return pltpu.VMEM(shape, dtype)

    level = [(rows >> l, cols >> l) for l in range(5)]
    scratch = [
        vmem(rows, cols), vmem(rows, words, dtype=jnp.int32),
        vmem(2 * HALO, cols), vmem(2 * HALO, words, dtype=jnp.int32),
        vmem(2 * packed, LANES), vmem(2 * packed, LANES),
        vmem(2 * packed, LANES), vmem(2 * packed, LANES),
        vmem(4 * HALO, LANES), vmem(4 * HALO, words, dtype=jnp.int32),
        vmem(blocks * ROW_CHUNK, 512, dtype=BF16), vmem(blocks * ROW_CHUNK, 256, dtype=BF16),
        vmem(blocks * ROW_CHUNK, 256), vmem(blocks * ROW_CHUNK, 256),
        vmem(rows + 2 * HALO, 256, dtype=BF16), vmem(rows + 2 * HALO, LANES, dtype=BF16),
        vmem(rows + 2 * HALO, 256), vmem(rows + 2 * HALO, 256),
        vmem(blocks + 1, rows + 2 * PAD, LANES), vmem(blocks + 1, rows + 2 * PAD, LANES),
        vmem(-(-(rows + 2 * PAD) // LANES) * LANES, LANES),
    ]
    for l in range(1, 4):
        scratch += [vmem(level[l][1] // LANES + 1, level[l][0] + 2 * PAD, LANES)] * 2
    count = level[2][0] + HALO
    inner_blocks = level[2][1] // LANES
    scratch += [
        vmem(2 * inner_blocks * count, 512, dtype=BF16), vmem(2 * count, 256, dtype=BF16),
        vmem(2 * inner_blocks * count, 256), vmem(2 * count, 256),
        vmem(512, 256, dtype=BF16), vmem(256, 256, dtype=BF16),
        vmem(8, LANES), vmem(8, LANES),
        vmem(n_cols, 8, LANES), vmem(n_rows, 8, LANES),
        pltpu.SemaphoreType.DMA((3 + chunks,)),
        pltpu.SemaphoreType.DMA((14,)), pltpu.SemaphoreType.DMA((14,)),
        pltpu.SemaphoreType.DMA((n_cols,)), pltpu.SemaphoreType.DMA((n_cols,)),
        pltpu.SemaphoreType.DMA((n_rows,)), pltpu.SemaphoreType.DMA((n_rows,)),
    ]
    out_shape = [jax.ShapeDtypeStruct(level[l], F32) for l in range(1, 5)]
    out_shape.append(jax.ShapeDtypeStruct((8, LANES), F32))
    v1, v2, v3, v4, stats = pl.pallas_call(
        kernel,
        out_shape=out_shape,
        in_specs=[pl.BlockSpec(memory_space=pl.ANY)] * 2,
        out_specs=[pl.BlockSpec(memory_space=pltpu.VMEM)] * 5,
        scratch_shapes=scratch,
        compiler_params=pltpu.CompilerParams(
            collective_id=0, has_side_effects=True, vmem_limit_bytes=48 * 1024 * 1024
        ),
    )(surface_field, land_words)
    return v1, v2, v3, v4, stats[0, :4], stats[1, :4]


def solution(mesh):
    spec = P("rows", "cols")
    return jax.shard_map(
        per_device, mesh=mesh, in_specs=(spec, spec),
        out_specs=(spec, spec, spec, spec, P(), P()), check_vma=False,
    )
```

```python
import math

import jax
import jax.numpy as jnp
from jax import lax
from jax.experimental import pallas as pl
from jax.experimental.pallas import tpu as pltpu
from jax.sharding import PartitionSpec as P

MESH = pl.DeviceIdType.MESH
F32 = jnp.float32
BF16 = jnp.bfloat16
HALO = 16
PAD = 24
LANES = 128
ROW_CHUNK = 64
FLOOR = 0.05
EPS = 1e-06


def lane_iota(rows, dtype=jnp.int32):
    return lax.broadcasted_iota(dtype, (rows, LANES), 1)


def tap_weight(offset):
    inner = jnp.logical_or(offset == 1, offset == 2)
    outer = jnp.logical_or(offset == 0, offset == 3)
    return jnp.where(inner, 0.375, jnp.where(outer, 0.125, 0.0))


def build_tables(band, edge):
    k = lax.broadcasted_iota(jnp.int32, (256, 256), 0)
    n = lax.broadcasted_iota(jnp.int32, (256, 256), 1)
    own = tap_weight(k - (2 * n - 1))
    spill = jnp.logical_or(
        jnp.logical_and(n == 128, k == 255), jnp.logical_and(n == 255, k == 0)
    )
    table = jnp.where(n < 128, own, jnp.where(spill, 0.125, 0.0)).astype(BF16)
    band[0:256, :] = table
    band[256:512, :] = table
    k = lax.broadcasted_iota(jnp.int32, (128, 256), 0)
    n = lax.broadcasted_iota(jnp.int32, (128, 256), 1)
    right = jnp.where(k < 64, tap_weight(k - (2 * n - 1)), 0.0)
    left = jnp.where(k >= 64, tap_weight(k - (2 * n - 129)), 0.0)
    spill = jnp.logical_or(
        jnp.logical_and(n == 128, k == 127), jnp.logical_and(n == 255, k == 0)
    )
    table = jnp.where(
        n < 64, right, jnp.where(n < 128, left, jnp.where(spill, 0.125, 0.0))
    ).astype(BF16)
    edge[0:128, :] = table
    edge[128:256, :] = table


def pieces(x):
    high = x.astype(BF16)
    low = (x - high.astype(F32)).astype(BF16)
    return high, low


def land_of(words, tile):
    rows = words.shape[0]
    lane = lane_iota(rows)
    picked = jnp.take_along_axis(
        words, 4 * tile + lane // 32, axis=1, mode="promise_in_bounds"
    )
    return jnp.left_shift(picked, 31 - lane % 32) < 0


def dot(a, b):
    return jnp.dot(a, b, preferred_element_type=F32)


def first_across(field_tile, words, rows, s_num, s_den, r_num, r_den, band, tiles, store):
    for tile in range(tiles):
        land = land_of(words, tile)
        masked = jnp.where(land, field_tile(tile), 0.0)
        high, low = pieces(masked)
        at = (tile // 2) * rows
        half = (tile % 2) * LANES
        s_num[at : at + rows, half : half + LANES] = high
        s_num[at : at + rows, 256 + half : 256 + half + LANES] = low
        s_den[at : at + rows, half : half + LANES] = jnp.where(land, 1.0, 0.0).astype(BF16)
    blocks = tiles // 2
    r_num[0 : blocks * rows, :] = dot(s_num[0 : blocks * rows, :], band[...])
    r_den[0 : blocks * rows, :] = dot(s_den[0 : blocks * rows, :], band[0:256, :])
    low_half = lane_iota(rows) < 64
    for which, ref in ((0, r_num), (1, r_den)):
        def spill(block):
            if block < 0 or block >= blocks:
                return jnp.zeros((rows, LANES), F32)
            return ref[block * rows : (block + 1) * rows, LANES : 2 * LANES]

        for block in range(blocks):
            own = ref[block * rows : (block + 1) * rows, 0:LANES]
            store(which, block, own + jnp.where(low_half, spill(block - 1), spill(block + 1)))
        store(which, blocks, jnp.where(low_half, spill(blocks - 1), spill(0)))


def kernel(
    field_hbm, words_hbm,
    v1, v2, v3, v4, stats,
    fld, wrd_cols, wrd, fhal, whal, out_left, out_right, in_left, in_right, cornf, cornw,
    s_num, s_den, r_num, r_den, se_num, se_den, re_num, re_den,
    hn, hd, cosb, p1, d1, p2, d2, p3, d3,
    sx, sxe, rx, rxe, band, edge, msg_a, msg_b, slot_a, slot_b,
    load_sem, send_sem, recv_sem, a_send, a_recv, b_send, b_recv,
):
    n_rows, n_cols = lax.axis_size("rows"), lax.axis_size("cols")
    my_row, my_col = lax.axis_index("rows"), lax.axis_index("cols")
    rows, cols = fld.shape
    tiles = cols // LANES
    up, down = lax.rem(my_row + n_rows - 1, n_rows), lax.rem(my_row + 1, n_rows)
    left, right = lax.rem(my_col + n_cols - 1, n_cols), lax.rem(my_col + 1, n_cols)

    barrier = pltpu.get_barrier_semaphore()
    peers = [(my_row, lax.rem(my_col + s, n_cols)) for s in range(1, n_cols)]
    peers += [(lax.rem(my_row + s, n_rows), my_col) for s in range(1, n_rows)]
    peers += [(up, left), (up, right), (down, left), (down, right)]
    for peer in peers:
        pl.semaphore_signal(barrier, inc=1, device_id=peer, device_id_type=MESH)

    loads = []

    def load(src, dst):
        copy = pltpu.make_async_copy(src, dst, load_sem.at[len(loads)])
        copy.start()
        loads.append(copy)
        return copy

    load_words = load(words_hbm, wrd_cols)
    load_strips = [
        load(field_hbm.at[:, 0:LANES], fld.at[:, 0:LANES]),
        load(field_hbm.at[:, cols - LANES : cols], fld.at[:, cols - LANES : cols]),
    ]
    chunks = rows // ROW_CHUNK
    order = [0, chunks - 1] + list(range(1, chunks - 1))
    load_chunk = {}
    for c in order:
        at = pl.ds(c * ROW_CHUNK, ROW_CHUNK)
        load_chunk[c] = load(
            field_hbm.at[at, LANES : cols - LANES], fld.at[at, LANES : cols - LANES]
        )

    build_tables(band, edge)
    for ref in (hn, hd, p1, d1, p2, d2, p3, d3):
        spare = PAD - HALO if ref.shape[1] == rows + 2 * PAD else HALO
        zeros = jnp.zeros((ref.shape[0], spare, LANES), F32)
        ref[:, 0:spare, :] = zeros
        ref[:, ref.shape[1] - spare :, :] = zeros

    sub = lax.broadcasted_iota(jnp.int32, (8, LANES), 0)
    global_row = my_row * rows - PAD + sub * LANES + lane_iota(8)
    latitude = ((global_row.astype(F32) + 0.5) / (rows * n_rows) - 0.5) * math.pi
    on_globe = jnp.logical_and(global_row >= 0, global_row < rows * n_rows)
    cosines = jnp.where(on_globe, jnp.cos(latitude) * 0.125, 0.0)
    for q in range(cosb.shape[0] // LANES):
        row = jnp.broadcast_to(cosines[q : q + 1, :], (LANES, LANES))
        cosb[q * LANES : (q + 1) * LANES, :] = jnp.transpose(row)

    load_words.wait()
    copies_of = LANES // wrd_cols.shape[0]
    for q in range(rows // LANES):
        at = slice(q * LANES, (q + 1) * LANES)
        wrd[at, :] = jnp.transpose(jnp.concatenate([wrd_cols[:, at]] * copies_of, axis=0))

    for copy in load_strips:
        copy.wait()
    packed = rows // 8
    lane = lane_iota(packed)
    for out, tile, shift in ((out_left, 0, 0), (out_right, tiles - 1, HALO)):
        field_part = jnp.zeros((packed, LANES), F32)
        land_part = jnp.zeros((packed, LANES), F32)
        for g in range(8):
            at = slice(g * packed, (g + 1) * packed)
            values = fld[at, tile * LANES : (tile + 1) * LANES]
            land = jnp.where(land_of(wrd[at, :], tile), 1.0, 0.0)
            turn = (HALO * g + shift) % LANES
            if turn:
                values, land = pltpu.roll(values, turn, 1), pltpu.roll(land, turn, 1)
            here = lane // HALO == g
            field_part = jnp.where(here, values, field_part)
            land_part = jnp.where(here, land, land_part)
        out[0:packed, :] = field_part
        out[packed : 2 * packed, :] = land_part
    load_chunk[0].wait()
    if chunks > 1:
        load_chunk[chunks - 1].wait()

    pl.semaphore_wait(barrier, len(peers))

    sends = []

    def send(src, dst, row, col):
        i = len(sends)
        copy = pltpu.make_async_remote_copy(
            src_ref=src, dst_ref=dst, send_sem=send_sem.at[i], recv_sem=recv_sem.at[i],
            device_id=(row, col), device_id_type=MESH,
        )
        copy.start()
        sends.append(copy)

    top, bottom = slice(0, HALO), slice(rows - HALO, rows)
    last_tile = slice(cols - LANES, cols)
    send(out_left, in_right, my_row, left)
    send(out_right, in_left, my_row, right)
    send(fld.at[top, :], fhal.at[HALO : 2 * HALO, :], up, my_col)
    send(fld.at[bottom, :], fhal.at[0:HALO, :], down, my_col)
    send(wrd.at[top, :], whal.at[HALO : 2 * HALO, :], up, my_col)
    send(wrd.at[bottom, :], whal.at[0:HALO, :], down, my_col)
    send(fld.at[bottom, last_tile], cornf.at[0 * HALO : 1 * HALO, :], down, right)
    send(fld.at[bottom, 0:LANES], cornf.at[1 * HALO : 2 * HALO, :], down, left)
    send(fld.at[top, last_tile], cornf.at[2 * HALO : 3 * HALO, :], up, right)
    send(fld.at[top, 0:LANES], cornf.at[3 * HALO : 4 * HALO, :], up, left)
    send(wrd.at[bottom, :], cornw.at[0 * HALO : 1 * HALO, :], down, right)
    send(wrd.at[bottom, :], cornw.at[1 * HALO : 2 * HALO, :], down, left)
    send(wrd.at[top, :], cornw.at[2 * HALO : 3 * HALO, :], up, right)
    send(wrd.at[top, :], cornw.at[3 * HALO : 4 * HALO, :], up, left)

    for c in order[2:]:
        load_chunk[c].wait()

    def own_rows(c, carry):
        at = pl.multiple_of(c * ROW_CHUNK, ROW_CHUNK)

        def field_tile(tile):
            return fld[pl.ds(at, ROW_CHUNK), tile * LANES : (tile + 1) * LANES]

        def store(which, tile, value):
            ref = (hn, hd)[which]
            ref[tile, pl.ds(PAD + at, ROW_CHUNK), :] = value

        first_across(
            field_tile, wrd[pl.ds(at, ROW_CHUNK), :], ROW_CHUNK,
            s_num, s_den, r_num, r_den, band, tiles, store,
        )
        return carry

    lax.fori_loop(0, chunks, own_rows, 0)

    for copy in sends:
        copy.wait()

    def halo_store(which, tile, value):
        ref = (hn, hd)[which]
        ref[tile, PAD - HALO : PAD, :] = value[0:HALO, :]
        ref[tile, PAD + rows : PAD + rows + HALO, :] = value[HALO : 2 * HALO, :]

    first_across(
        lambda tile: fhal[:, tile * LANES : (tile + 1) * LANES], whal[...], 2 * HALO,
        s_num, s_den, r_num, r_den, band, tiles, halo_store,
    )

    def edge_store(at, count, field_value, land_value):
        high, low = pieces(field_value * land_value)
        se_num[at : at + count, 0:LANES] = high
        se_num[at : at + count, LANES : 2 * LANES] = low
        se_den[at : at + count, :] = land_value.astype(BF16)

    for g in range(8):
        parts = []
        for base in (0, packed):
            from_right = in_right[base : base + packed, :]
            from_left = in_left[base : base + packed, :]
            turn = (LANES - HALO * g) % LANES
            if turn:
                from_right = pltpu.roll(from_right, turn, 1)
            turn = (LANES - HALO - HALO * g) % LANES
            if turn:
                from_left = pltpu.roll(from_left, turn, 1)
            parts.append(
                jnp.where(
                    lane < HALO, from_right, jnp.where(lane >= LANES - HALO, from_left, 0.0)
                )
            )
        edge_store(g * packed, packed, parts[0], parts[1])
    lane16 = lane_iota(HALO)
    for side in range(2):
        l_at = slice(2 * side * HALO, (2 * side + 1) * HALO)
        r_at = slice((2 * side + 1) * HALO, (2 * side + 2) * HALO)
        is_right, is_left = lane16 < HALO, lane16 >= LANES - HALO
        value = jnp.where(is_right, cornf[r_at, :], jnp.where(is_left, cornf[l_at, :], 0.0))
        land_r = jnp.where(land_of(cornw[r_at, :], 0), 1.0, 0.0)
        land_l = jnp.where(land_of(cornw[l_at, :], tiles - 1), 1.0, 0.0)
        land = jnp.where(is_right, land_r, jnp.where(is_left, land_l, 0.0))
        edge_store(rows + side * HALO, HALO, value, land)
    re_num[...] = dot(se_num[...], edge[...])
    re_den[...] = dot(se_den[...], edge[0:128, :])
    out_tiles = tiles // 2

    def merge_edge(src, dst, count):
        low_half = lane_iota(count) < 64
        for result, ref in ((re_num, hn), (re_den, hd)):
            spill = result[pl.ds(src, count), LANES : 2 * LANES]
            here = pl.ds(dst, count)
            last = out_tiles - 1
            ref[0, here, :] = ref[0, here, :] + jnp.where(low_half, spill, 0.0)
            ref[last, here, :] = ref[last, here, :] + jnp.where(low_half, 0.0, spill)
            ref[out_tiles, here, :] = ref[out_tiles, here, :] + result[pl.ds(src, count), 0:LANES]

    def merge_own(c, carry):
        at = pl.multiple_of(c * ROW_CHUNK, ROW_CHUNK)
        merge_edge(at, PAD + at, ROW_CHUNK)
        return carry

    lax.fori_loop(0, chunks, merge_own, 0)
    merge_edge(rows, PAD - HALO, HALO)
    merge_edge(rows + HALO, PAD + rows, HALO)

    inside_top, inside_bottom = my_row > 0, my_row < n_rows - 1
    out_rows = rows // 2

    def finish(num, den):
        value = num / jnp.maximum(den, FLOOR)
        return value, den * value

    def level_one_rows(i0, tile, cosine):
        result = []
        for ref in (hn, hd):
            taps = [ref[tile, pl.ds(PAD + 2 * i0 - 1 + a, 8, stride=2), :] for a in range(4)]
            taps = [t * c for t, c in zip(taps, cosine)]
            result.append((taps[0] + taps[3]) + (taps[1] + taps[2]))
        return result

    def cosine_of(i0):
        taps = [cosb[pl.ds(PAD + 2 * i0 - 1 + a, 8, stride=2), :] for a in range(4)]
        return [taps[0], 3.0 * taps[1], 3.0 * taps[2], taps[3]]

    zero_sums = (
        jnp.zeros((8, LANES), F32), jnp.zeros((8, LANES), F32), jnp.full((8, LANES), -jnp.inf, F32)
    )

    def gather_sums(sums, value, product, cover):
        return (sums[0] + product, sums[1] + cover, jnp.maximum(sums[2], value))

    def level_one(c, sums):
        i0 = pl.multiple_of(c * 8, 8)
        cosine = cosine_of(i0)
        for tile in range(out_tiles + 1):
            at = slice(tile * LANES, (tile + 1) * LANES)
            num, den = level_one_rows(i0, tile, cosine)
            value, product = finish(num, den)
            p1[tile, pl.ds(PAD + i0, 8), :] = product
            d1[tile, pl.ds(PAD + i0, 8), :] = den
            if tile < out_tiles:
                v1[pl.ds(i0, 8), at] = value
                sums = gather_sums(sums, value, product, den)
        return sums

    all_sums = [lax.fori_loop(0, out_rows // 8, level_one, zero_sums)]
    for i0, keep in ((-8, inside_top), (out_rows, inside_bottom)):
        cosine = cosine_of(i0)
        for tile in range(out_tiles + 1):
            num, den = level_one_rows(i0, tile, cosine)
            value, product = finish(num, den)
            p1[tile, PAD + i0 : PAD + i0 + 8, :] = jnp.where(keep, product, 0.0)
            d1[tile, PAD + i0 : PAD + i0 + 8, :] = jnp.where(keep, den, 0.0)

    def next_level(pin, din, pout, dout, vout):
        out_rows, out_cols = vout.shape
        blocks = out_cols // LANES
        last_level = pout is None
        count = out_rows if last_level else out_rows + HALO

        def down_rows(ref, i0, size, tile):
            taps = [ref[tile, pl.ds(PAD + 2 * i0 - 1 + a, size, stride=2), :] for a in range(4)]
            return 0.125 * (taps[0] + taps[3]) + 0.375 * (taps[1] + taps[2])

        def put(which, tile, m0, value):
            high, low = pieces(value)
            if tile < 2 * blocks:
                base = (which * blocks + tile // 2) * count + m0
                half = (tile % 2) * LANES
                sx[pl.ds(base, 16), half : half + LANES] = high
                sx[pl.ds(base, 16), 256 + half : 256 + half + LANES] = low
            else:
                base = which * count + m0
                sxe[pl.ds(base, 16), 0:LANES] = high
                sxe[pl.ds(base, 16), LANES : 2 * LANES] = low

        def rows_step(c, carry):
            i0 = pl.multiple_of(c * 16, 16)
            for which, ref in ((0, pin), (1, din)):
                for tile in range(2 * blocks + 1):
                    value = jnp.concatenate(
                        [down_rows(ref, i0, 8, tile), down_rows(ref, i0 + 8, 8, tile)], axis=0
                    )
                    put(which, tile, i0, value)
            return carry

        lax.fori_loop(0, out_rows // 16, rows_step, 0)
        if not last_level:
            for which, ref in ((0, pin), (1, din)):
                for tile in range(2 * blocks + 1):
                    value = jnp.concatenate(
                        [down_rows(ref, -8, 8, tile), down_rows(ref, out_rows, 8, tile)], axis=0
                    )
                    put(which, tile, out_rows, value)
        total = 2 * blocks * count
        rx[0:total, :] = dot(sx[0:total, :], band[...])
        rxe[0 : 2 * count, :] = dot(sxe[0 : 2 * count, :], edge[...])
        low_half = lane_iota(8) < 64

        def across(m0, tile):
            result = []
            for which in range(2):
                def piece(block, half):
                    block = block % (blocks + 1)
                    at = slice(half * LANES, (half + 1) * LANES)
                    if block == blocks:
                        return rxe[pl.ds(which * count + m0, 8), at]
                    return rx[pl.ds((which * blocks + block) * count + m0, 8), at]

                result.append(
                    piece(tile, 0)
                    + jnp.where(low_half, piece(tile - 1, 1), piece(tile + 1, 1))
                )
            return result

        def finish_step(c, sums):
            i0 = pl.multiple_of(c * 8, 8)
            for tile in range(blocks + (0 if last_level else 1)):
                at = slice(tile * LANES, (tile + 1) * LANES)
                num, den = across(i0, tile)
                value, product = finish(num, den)
                if not last_level:
                    pout[tile, pl.ds(PAD + i0, 8), :] = product
                    dout[tile, pl.ds(PAD + i0, 8), :] = den
                if tile < blocks:
                    vout[pl.ds(i0, 8), at] = value
                    sums = gather_sums(sums, value, product, den)
            return sums

        sums = lax.fori_loop(0, out_rows // 8, finish_step, zero_sums)
        if not last_level:
            for m0, i0, keep in (
                (out_rows, -8, inside_top), (out_rows + 8, out_rows, inside_bottom)
            ):
                for tile in range(blocks + 1):
                    num, den = across(m0, tile)
                    value, product = finish(num, den)
                    pout[tile, PAD + i0 : PAD + i0 + 8, :] = jnp.where(keep, product, 0.0)
                    dout[tile, PAD + i0 : PAD + i0 + 8, :] = jnp.where(keep, den, 0.0)
        return sums

    all_sums.append(next_level(p1, d1, p2, d2, v2))
    all_sums.append(next_level(p2, d2, p3, d3, v3))
    all_sums.append(next_level(p3, d3, None, None, v4))

    lane = lane_iota(1)
    message = jnp.zeros((1, LANES), F32)

    def whole(x, op):
        return op(op(x, axis=0, keepdims=True), axis=1, keepdims=True)

    for level, sums in enumerate(all_sums):
        for place, (part, op) in enumerate(zip(sums, (jnp.sum, jnp.sum, jnp.max))):
            message = jnp.where(lane == 4 * place + level, whole(part, op), message)

    def exchange(message, buffer, slots, send_sems, recv_sems, index, count, device):
        buffer[...] = message
        slots[index] = message
        copies = []
        for s in range(1, count):
            peer = lax.rem(index + s, count)
            copy = pltpu.make_async_remote_copy(
                src_ref=buffer, dst_ref=slots.at[index],
                send_sem=send_sems.at[s], recv_sem=recv_sems.at[index],
                device_id=device(peer), device_id_type=MESH,
            )
            copy.start()
            copies.append(copy)
        for s in range(1, count):
            peer = lax.rem(index + s, count)
            pltpu.make_async_remote_copy(
                src_ref=buffer, dst_ref=slots.at[peer],
                send_sem=send_sems.at[s], recv_sem=recv_sems.at[peer],
                device_id=device(peer), device_id_type=MESH,
            ).wait_recv()
        added, largest = slots[0], slots[0]
        for i in range(1, count):
            added, largest = added + slots[i], jnp.maximum(largest, slots[i])
        for copy in copies:
            copy.wait_send()
        return jnp.where(lane < 8, added, largest)

    message = exchange(
        message, msg_b, slot_b, b_send, b_recv, my_row, n_rows, lambda peer: (peer, my_col)
    )
    message = exchange(
        message, msg_a, slot_a, a_send, a_recv, my_col, n_cols, lambda peer: (my_row, peer)
    )
    wide = jnp.broadcast_to(message, (8, LANES))
    covers = pltpu.roll(wide, LANES - 4, 1)
    maxima = pltpu.roll(wide, LANES - 8, 1)
    stats[...] = jnp.where(sub == 0, wide / (covers + EPS), maxima)


def copy_out(v1, v2, v3, v4, stats):
    def body(*refs):
        ins, outs, means, maxima, sem = refs[:5], refs[5:9], refs[9], refs[10], refs[11]
        copies = []
        for i in range(4):
            copy = pltpu.make_async_copy(ins[i], outs[i], sem.at[i])
            copy.start()
            copies.append(copy)
        for i in range(4):
            means[i] = ins[4][0, i]
            maxima[i] = ins[4][1, i]
        for copy in copies:
            copy.wait()

    shapes = [jax.ShapeDtypeStruct(v.shape, F32) for v in (v1, v2, v3, v4)]
    shapes += [jax.ShapeDtypeStruct((4,), F32)] * 2
    return pl.pallas_call(
        body,
        out_shape=shapes,
        in_specs=[pl.BlockSpec(memory_space=pltpu.VMEM)] * 5,
        out_specs=[pl.BlockSpec(memory_space=pl.ANY)] * 4
        + [pl.BlockSpec(memory_space=pltpu.SMEM)] * 2,
        scratch_shapes=[pltpu.SemaphoreType.DMA((4,))],
    )(*[pltpu.with_memory_space_constraint(x, pltpu.VMEM) for x in (v1, v2, v3, v4, stats)])


def per_device(surface_field, land_words):
    rows, cols = surface_field.shape
    n_rows, n_cols = lax.axis_size("rows"), lax.axis_size("cols")
    words = land_words.shape[1]
    chunks = rows // ROW_CHUNK
    blocks = cols // 256
    packed = rows // 8

    def vmem(*shape, dtype=F32):
        return pltpu.VMEM(shape, dtype)

    level = [(rows >> l, cols >> l) for l in range(5)]
    scratch = [
        vmem(rows, cols), vmem(words, rows, dtype=jnp.int32), vmem(rows, LANES, dtype=jnp.int32),
        vmem(2 * HALO, cols), vmem(2 * HALO, LANES, dtype=jnp.int32),
        vmem(2 * packed, LANES), vmem(2 * packed, LANES),
        vmem(2 * packed, LANES), vmem(2 * packed, LANES),
        vmem(4 * HALO, LANES), vmem(4 * HALO, LANES, dtype=jnp.int32),
        vmem(blocks * ROW_CHUNK, 512, dtype=BF16), vmem(blocks * ROW_CHUNK, 256, dtype=BF16),
        vmem(blocks * ROW_CHUNK, 256), vmem(blocks * ROW_CHUNK, 256),
        vmem(rows + 2 * HALO, 256, dtype=BF16), vmem(rows + 2 * HALO, LANES, dtype=BF16),
        vmem(rows + 2 * HALO, 256), vmem(rows + 2 * HALO, 256),
        vmem(blocks + 1, rows + 2 * PAD, LANES), vmem(blocks + 1, rows + 2 * PAD, LANES),
        vmem(-(-(rows + 2 * PAD) // LANES) * LANES, LANES),
    ]
    for l in range(1, 4):
        scratch += [vmem(level[l][1] // LANES + 1, level[l][0] + 2 * PAD, LANES)] * 2
    count = level[2][0] + HALO
    inner_blocks = level[2][1] // LANES
    scratch += [
        vmem(2 * inner_blocks * count, 512, dtype=BF16), vmem(2 * count, 256, dtype=BF16),
        vmem(2 * inner_blocks * count, 256), vmem(2 * count, 256),
        vmem(512, 256, dtype=BF16), vmem(256, 256, dtype=BF16),
        vmem(1, LANES), vmem(1, LANES),
        vmem(n_cols, 1, LANES), vmem(n_rows, 1, LANES),
        pltpu.SemaphoreType.DMA((3 + chunks,)),
        pltpu.SemaphoreType.DMA((14,)), pltpu.SemaphoreType.DMA((14,)),
        pltpu.SemaphoreType.DMA((n_cols,)), pltpu.SemaphoreType.DMA((n_cols,)),
        pltpu.SemaphoreType.DMA((n_rows,)), pltpu.SemaphoreType.DMA((n_rows,)),
    ]
    out_shape = [pltpu.VMEM(level[l], F32) for l in range(1, 5)]
    out_shape.append(pltpu.VMEM((8, LANES), F32))
    v1, v2, v3, v4, stats = pl.pallas_call(
        kernel,
        out_shape=out_shape,
        in_specs=[pl.BlockSpec(memory_space=pl.ANY)] * 2,
        out_specs=[pl.BlockSpec(memory_space=pltpu.VMEM)] * 5,
        scratch_shapes=scratch,
        compiler_params=pltpu.CompilerParams(
            collective_id=0, has_side_effects=True, vmem_limit_bytes=48 * 1024 * 1024
        ),
    )(
        pltpu.with_memory_space_constraint(surface_field, pltpu.HBM),
        pltpu.with_memory_space_constraint(land_words.T, pltpu.HBM),
    )
    return copy_out(v1, v2, v3, v4, stats)


def solution(mesh):
    spec = P("rows", "cols")
    return jax.shard_map(
        per_device, mesh=mesh, in_specs=(spec, spec),
        out_specs=(spec, spec, spec, spec, P(), P()), check_vma=False,
    )
```

```python
import math

import jax
import jax.numpy as jnp
from jax import lax
from jax.experimental import pallas as pl
from jax.experimental.pallas import tpu as pltpu
from jax.sharding import PartitionSpec as P

MESH = pl.DeviceIdType.MESH
F32 = jnp.float32
BF16 = jnp.bfloat16
HALO = 16
PAD = 24
LANES = 128
ROW_CHUNK = 64
FLOOR = 0.05
EPS = 1e-06


def lane_iota(rows, dtype=jnp.int32):
    return lax.broadcasted_iota(dtype, (rows, LANES), 1)


def tap_weight(offset):
    inner = jnp.logical_or(offset == 1, offset == 2)
    outer = jnp.logical_or(offset == 0, offset == 3)
    return jnp.where(inner, 0.375, jnp.where(outer, 0.125, 0.0))


def build_tables(band, edge):
    k = lax.broadcasted_iota(jnp.int32, (256, 256), 0)
    n = lax.broadcasted_iota(jnp.int32, (256, 256), 1)
    own = tap_weight(k - (2 * n - 1))
    spill = jnp.logical_or(
        jnp.logical_and(n == 128, k == 255), jnp.logical_and(n == 255, k == 0)
    )
    table = jnp.where(n < 128, own, jnp.where(spill, 0.125, 0.0))
    band[0:256, :] = table.astype(BF16)
    band[256:512, :] = table.astype(BF16)
    k = lax.broadcasted_iota(jnp.int32, (128, 256), 0)
    n = lax.broadcasted_iota(jnp.int32, (128, 256), 1)
    right = jnp.where(k < 64, tap_weight(k - (2 * n - 1)), 0.0)
    left = jnp.where(k >= 64, tap_weight(k - (2 * n - 129)), 0.0)
    spill = jnp.logical_or(
        jnp.logical_and(n == 128, k == 127), jnp.logical_and(n == 255, k == 0)
    )
    table = jnp.where(
        n < 64, right, jnp.where(n < 128, left, jnp.where(spill, 0.125, 0.0))
    ).astype(BF16)
    edge[0:128, :] = table
    edge[128:256, :] = table


def pieces(x):
    high = x.astype(BF16)
    low = (x - high.astype(F32)).astype(BF16)
    return high, low


def land_of(words, tile):
    rows = words.shape[0]
    lane = lane_iota(rows)
    picked = jnp.take_along_axis(
        words, 4 * tile + lane // 32, axis=1, mode="promise_in_bounds"
    )
    return jnp.left_shift(picked, 31 - lane % 32) < 0


def dot(a, b):
    return jnp.dot(a, b, preferred_element_type=F32)


def mask_step(field_tile, words, rows, s_num, s_den, tiles):
    for tile in range(tiles):
        land = land_of(words, tile)
        masked = jnp.where(land, field_tile(tile), 0.0)
        at = (tile // 2) * rows
        half = (tile % 2) * LANES
        high, low = pieces(masked)
        s_num[at : at + rows, half : half + LANES] = high
        s_num[at : at + rows, 256 + half : 256 + half + LANES] = low
        s_den[at : at + rows, half : half + LANES] = jnp.where(land, 1.0, 0.0).astype(BF16)


def across_step(rows, s_num, s_den, r_num, r_den, band, tiles, store):
    blocks = tiles // 2
    r_num[0 : blocks * rows, :] = dot(s_num[0 : blocks * rows, :], band[...])
    r_den[0 : blocks * rows, :] = dot(s_den[0 : blocks * rows, :], band[0:256, :])
    low_half = lane_iota(rows) < 64
    for which, ref in ((0, r_num), (1, r_den)):
        def spill(block):
            if block < 0 or block >= blocks:
                return jnp.zeros((rows, LANES), F32)
            return ref[block * rows : (block + 1) * rows, LANES : 2 * LANES]

        for block in range(blocks):
            own = ref[block * rows : (block + 1) * rows, 0:LANES]
            store(which, block, own + jnp.where(low_half, spill(block - 1), spill(block + 1)))
        store(which, blocks, jnp.where(low_half, spill(blocks - 1), spill(0)))


def first_across(field_tile, words, rows, s_num, s_den, r_num, r_den, band, tiles, store):
    mask_step(field_tile, words, rows, s_num, s_den, tiles)
    across_step(rows, s_num, s_den, r_num, r_den, band, tiles, store)


def kernel(
    field_hbm, words_hbm,
    v1, v2, v3, v4, stats,
    fld, wrd_cols, wrd, fhal, whal, out_left, out_right, in_left, in_right, cornf, cornw,
    s_num, s_den, r_num, r_den, s_num2, s_den2, r_num2, r_den2, se_num, se_den, re_num, re_den,
    hn, hd, cosb, p1, d1, p2, d2, p3, d3,
    sx, sxe, rx, rxe, band, edge, msg_a, msg_b, slot_a, slot_b,
    load_sem, send_sem, recv_sem, a_send, a_recv, b_send, b_recv,
):
    n_rows, n_cols = lax.axis_size("rows"), lax.axis_size("cols")
    my_row, my_col = lax.axis_index("rows"), lax.axis_index("cols")
    rows, cols = fld.shape
    tiles = cols // LANES
    up, down = lax.rem(my_row + n_rows - 1, n_rows), lax.rem(my_row + 1, n_rows)
    left, right = lax.rem(my_col + n_cols - 1, n_cols), lax.rem(my_col + 1, n_cols)

    barrier = pltpu.get_barrier_semaphore()
    peers = [(my_row, lax.rem(my_col + s, n_cols)) for s in range(1, n_cols)]
    peers += [(lax.rem(my_row + s, n_rows), my_col) for s in range(1, n_rows)]
    peers += [(up, left), (up, right), (down, left), (down, right)]
    for peer in peers:
        pl.semaphore_signal(barrier, inc=1, device_id=peer, device_id_type=MESH)

    loads = []

    def load(src, dst):
        copy = pltpu.make_async_copy(src, dst, load_sem.at[len(loads)])
        copy.start()
        loads.append(copy)
        return copy

    load_words = load(words_hbm, wrd_cols)
    load_strips = [
        load(field_hbm.at[:, 0:LANES], fld.at[:, 0:LANES]),
        load(field_hbm.at[:, cols - LANES : cols], fld.at[:, cols - LANES : cols]),
    ]
    chunks = rows // ROW_CHUNK
    order = [0, chunks - 1] + list(range(1, chunks - 1))
    load_chunk = {}
    for c in order:
        at = pl.ds(c * ROW_CHUNK, ROW_CHUNK)
        load_chunk[c] = load(
            field_hbm.at[at, LANES : cols - LANES], fld.at[at, LANES : cols - LANES]
        )

    build_tables(band, edge)
    for ref in (hn, hd, p1, d1, p2, d2, p3, d3):
        spare = PAD - HALO if ref.shape[1] == rows + 2 * PAD else HALO
        zeros = jnp.zeros((ref.shape[0], spare, LANES), F32)
        ref[:, 0:spare, :] = zeros
        ref[:, ref.shape[1] - spare :, :] = zeros

    sub = lax.broadcasted_iota(jnp.int32, (8, LANES), 0)
    global_row = my_row * rows - PAD + sub * LANES + lane_iota(8)
    latitude = ((global_row.astype(F32) + 0.5) / (rows * n_rows) - 0.5) * math.pi
    on_globe = jnp.logical_and(global_row >= 0, global_row < rows * n_rows)
    cosines = jnp.where(on_globe, jnp.cos(latitude) * 0.125, 0.0)
    for q in range(cosb.shape[0] // LANES):
        row = jnp.broadcast_to(cosines[q : q + 1, :], (LANES, LANES))
        cosb[q * LANES : (q + 1) * LANES, :] = jnp.transpose(row)

    load_words.wait()
    copies_of = LANES // wrd_cols.shape[0]
    for q in range(rows // LANES):
        at = slice(q * LANES, (q + 1) * LANES)
        wrd[at, :] = jnp.transpose(jnp.concatenate([wrd_cols[:, at]] * copies_of, axis=0))

    for copy in load_strips:
        copy.wait()
    packed = rows // 8
    lane = lane_iota(packed)
    for out, tile, shift in ((out_left, 0, 0), (out_right, tiles - 1, HALO)):
        field_part = jnp.zeros((packed, LANES), F32)
        land_part = jnp.zeros((packed, LANES), F32)
        for g in range(8):
            at = slice(g * packed, (g + 1) * packed)
            values = fld[at, tile * LANES : (tile + 1) * LANES]
            land = jnp.where(land_of(wrd[at, :], tile), 1.0, 0.0)
            turn = (HALO * g + shift) % LANES
            if turn:
                values, land = pltpu.roll(values, turn, 1), pltpu.roll(land, turn, 1)
            here = lane // HALO == g
            field_part = jnp.where(here, values, field_part)
            land_part = jnp.where(here, land, land_part)
        out[0:packed, :] = field_part
        out[packed : 2 * packed, :] = land_part
    load_chunk[0].wait()
    if chunks > 1:
        load_chunk[chunks - 1].wait()

    pl.semaphore_wait(barrier, len(peers))

    sends = []

    def send(src, dst, row, col):
        i = len(sends)
        copy = pltpu.make_async_remote_copy(
            src_ref=src, dst_ref=dst, send_sem=send_sem.at[i], recv_sem=recv_sem.at[i],
            device_id=(row, col), device_id_type=MESH,
        )
        copy.start()
        sends.append(copy)

    top, bottom = slice(0, HALO), slice(rows - HALO, rows)
    last_tile = slice(cols - LANES, cols)
    send(out_left, in_right, my_row, left)
    send(out_right, in_left, my_row, right)
    send(fld.at[top, :], fhal.at[HALO : 2 * HALO, :], up, my_col)
    send(fld.at[bottom, :], fhal.at[0:HALO, :], down, my_col)
    send(wrd.at[top, :], whal.at[HALO : 2 * HALO, :], up, my_col)
    send(wrd.at[bottom, :], whal.at[0:HALO, :], down, my_col)
    send(fld.at[bottom, last_tile], cornf.at[0 * HALO : 1 * HALO, :], down, right)
    send(fld.at[bottom, 0:LANES], cornf.at[1 * HALO : 2 * HALO, :], down, left)
    send(fld.at[top, last_tile], cornf.at[2 * HALO : 3 * HALO, :], up, right)
    send(fld.at[top, 0:LANES], cornf.at[3 * HALO : 4 * HALO, :], up, left)
    send(wrd.at[bottom, :], cornw.at[0 * HALO : 1 * HALO, :], down, right)
    send(wrd.at[bottom, :], cornw.at[1 * HALO : 2 * HALO, :], down, left)
    send(wrd.at[top, :], cornw.at[2 * HALO : 3 * HALO, :], up, right)
    send(wrd.at[top, :], cornw.at[3 * HALO : 4 * HALO, :], up, left)

    for c in order[2:]:
        load_chunk[c].wait()

    sets = ((s_num, s_den, r_num, r_den), (s_num2, s_den2, r_num2, r_den2))

    def own_mask(at, which):
        def field_tile(tile):
            return fld[pl.ds(at, ROW_CHUNK), tile * LANES : (tile + 1) * LANES]

        mask_step(
            field_tile, wrd[pl.ds(at, ROW_CHUNK), :], ROW_CHUNK, *sets[which][0:2], tiles
        )

    def own_across(at, which):
        def store(which, tile, value):
            ref = (hn, hd)[which]
            ref[tile, pl.ds(PAD + at, ROW_CHUNK), :] = value

        across_step(ROW_CHUNK, *sets[which], band, tiles, store)

    own_mask(0, 0)
    for c in range(chunks):
        if c + 1 < chunks:
            own_mask((c + 1) * ROW_CHUNK, (c + 1) % 2)
        own_across(c * ROW_CHUNK, c % 2)

    inside_top, inside_bottom = my_row > 0, my_row < n_rows - 1
    out_rows, out_tiles = rows // 2, tiles // 2

    def finish(num, den):
        value = num / jnp.maximum(den, FLOOR)
        return value, den * value

    zero_sums = (
        jnp.zeros((8, LANES), F32), jnp.zeros((8, LANES), F32), jnp.full((8, LANES), -jnp.inf, F32)
    )

    def gather_sums(sums, value, product, cover):
        return (sums[0] + product, sums[1] + cover, jnp.maximum(sums[2], value))

    def level_one_rows(i0, tile, cosine):
        result = []
        for ref in (hn, hd):
            taps = [ref[tile, pl.ds(PAD + 2 * i0 - 1 + a, 8, stride=2), :] for a in range(4)]
            taps = [t * c for t, c in zip(taps, cosine)]
            result.append((taps[0] + taps[3]) + (taps[1] + taps[2]))
        return result

    def cosine_of(i0):
        taps = [cosb[pl.ds(PAD + 2 * i0 - 1 + a, 8, stride=2), :] for a in range(4)]
        return [taps[0], 3.0 * taps[1], 3.0 * taps[2], taps[3]]

    def level_one_own(i0, which_tiles, sums):
        cosine = cosine_of(i0)
        for tile in which_tiles:
            num, den = level_one_rows(i0, tile, cosine)
            value, product = finish(num, den)
            p1[tile, pl.ds(PAD + i0, 8), :] = product
            d1[tile, pl.ds(PAD + i0, 8), :] = den
            if tile < out_tiles:
                v1[pl.ds(i0, 8), tile * LANES : (tile + 1) * LANES] = value
                sums = gather_sums(sums, value, product, den)
        return sums

    def level_one_inner(which_tiles, sums):
        def pair(c, sums):
            i0 = pl.multiple_of(8 + c * 16, 8)
            sums = level_one_own(i0, which_tiles, sums)
            return level_one_own(i0 + 8, which_tiles, sums)

        return lax.fori_loop(0, out_rows // 16 - 1, pair, sums)

    def level_one_beyond(i0, keep):
        cosine = cosine_of(i0)
        for tile in range(out_tiles + 1):
            num, den = level_one_rows(i0, tile, cosine)
            value, product = finish(num, den)
            p1[tile, PAD + i0 : PAD + i0 + 8, :] = jnp.where(keep, product, 0.0)
            d1[tile, PAD + i0 : PAD + i0 + 8, :] = jnp.where(keep, den, 0.0)

    sums_one = level_one_inner(range(1, out_tiles - 1), zero_sums)

    for copy in sends[0:2]:
        copy.wait()

    def edge_store(at, count, field_value, land_value):
        high, low = pieces(field_value * land_value)
        se_num[at : at + count, 0:LANES] = high
        se_num[at : at + count, LANES : 2 * LANES] = low
        se_den[at : at + count, :] = land_value.astype(BF16)

    def edge_dot(at, count):
        here = slice(at, at + count)
        re_num[here, :] = dot(se_num[here, :], edge[...])
        re_den[here, :] = dot(se_den[here, :], edge[0:128, :])

    def merge_edge(src, dst, count):
        low_half = lane_iota(count) < 64
        for result, ref in ((re_num, hn), (re_den, hd)):
            spill = result[src : src + count, LANES : 2 * LANES]
            here = slice(dst, dst + count)
            last = out_tiles - 1
            ref[0, here, :] = ref[0, here, :] + jnp.where(low_half, spill, 0.0)
            ref[last, here, :] = ref[last, here, :] + jnp.where(low_half, 0.0, spill)
            ref[out_tiles, here, :] = (
                ref[out_tiles, here, :] + result[src : src + count, 0:LANES]
            )

    for g in range(8):
        parts = []
        for base in (0, packed):
            from_right = in_right[base : base + packed, :]
            from_left = in_left[base : base + packed, :]
            turn = (LANES - HALO * g) % LANES
            if turn:
                from_right = pltpu.roll(from_right, turn, 1)
            turn = (LANES - HALO - HALO * g) % LANES
            if turn:
                from_left = pltpu.roll(from_left, turn, 1)
            parts.append(
                jnp.where(
                    lane < HALO, from_right, jnp.where(lane >= LANES - HALO, from_left, 0.0)
                )
            )
        edge_store(g * packed, packed, parts[0], parts[1])
    edge_dot(0, rows)
    merge_edge(0, PAD, rows)
    sums_one = level_one_inner((0, out_tiles - 1, out_tiles), sums_one)

    for copy in sends[2:]:
        copy.wait()

    def halo_store(which, tile, value):
        ref = (hn, hd)[which]
        ref[tile, PAD - HALO : PAD, :] = value[0:HALO, :]
        ref[tile, PAD + rows : PAD + rows + HALO, :] = value[HALO : 2 * HALO, :]

    first_across(
        lambda tile: fhal[:, tile * LANES : (tile + 1) * LANES], whal[...], 2 * HALO,
        s_num, s_den, r_num, r_den, band, tiles, halo_store,
    )
    lane16 = lane_iota(HALO)
    for side in range(2):
        l_at = slice(2 * side * HALO, (2 * side + 1) * HALO)
        r_at = slice((2 * side + 1) * HALO, (2 * side + 2) * HALO)
        is_right, is_left = lane16 < HALO, lane16 >= LANES - HALO
        value = jnp.where(is_right, cornf[r_at, :], jnp.where(is_left, cornf[l_at, :], 0.0))
        land_r = jnp.where(land_of(cornw[r_at, :], 0), 1.0, 0.0)
        land_l = jnp.where(land_of(cornw[l_at, :], tiles - 1), 1.0, 0.0)
        land = jnp.where(is_right, land_r, jnp.where(is_left, land_l, 0.0))
        edge_store(rows + side * HALO, HALO, value, land)
    edge_dot(rows, 2 * HALO)
    merge_edge(rows, PAD - HALO, HALO)
    merge_edge(rows + HALO, PAD + rows, HALO)
    for i0 in (0, out_rows - 8):
        sums_one = level_one_own(i0, range(out_tiles + 1), sums_one)
    level_one_beyond(-8, inside_top)
    level_one_beyond(out_rows, inside_bottom)
    all_sums = [sums_one]

    def next_level(pin, din, pout, dout, vout):
        out_rows, out_cols = vout.shape
        blocks = out_cols // LANES
        last_level = pout is None
        groups = [(i0, i0 + 8) for i0 in range(0, out_rows, 16)]
        parts = [groups[i : i + 4] for i in range(0, len(groups), 4)]
        if not last_level:
            parts.append([(-8, out_rows)])
        low_half = lane_iota(8) < 64

        def down_rows(ref, i0, tile):
            taps = [ref[tile, pl.ds(PAD + 2 * i0 - 1 + a, 8, stride=2), :] for a in range(4)]
            return 0.125 * (taps[0] + taps[3]) + 0.375 * (taps[1] + taps[2])

        sums, base, base_e = zero_sums, 0, 0
        for part in parts:
            count = 16 * len(part)
            for g, pair in enumerate(part):
                for which, ref in ((0, pin), (1, din)):
                    for tile in range(2 * blocks + 1):
                        value = jnp.concatenate(
                            [down_rows(ref, i0, tile) for i0 in pair], axis=0
                        )
                        high, low = pieces(value)
                        if tile < 2 * blocks:
                            at = base + (which * blocks + tile // 2) * count + 16 * g
                            half = (tile % 2) * LANES
                            sx[at : at + 16, half : half + LANES] = high
                            sx[at : at + 16, 256 + half : 256 + half + LANES] = low
                        else:
                            at = base_e + which * count + 16 * g
                            sxe[at : at + 16, 0:LANES] = high
                            sxe[at : at + 16, LANES : 2 * LANES] = low
            total = 2 * blocks * count
            rx[base : base + total, :] = dot(sx[base : base + total, :], band[...])
            rxe[base_e : base_e + 2 * count, :] = dot(
                sxe[base_e : base_e + 2 * count, :], edge[...]
            )
            starts = [i0 for pair in part for i0 in pair]
            for m, i0 in enumerate(starts):
                beyond = i0 < 0 or i0 >= out_rows
                keep = inside_top if i0 < 0 else inside_bottom
                for tile in range(blocks + (0 if last_level else 1)):
                    both = []
                    for which in range(2):
                        def piece(block, half, which=which):
                            block = block % (blocks + 1)
                            lanes = slice(half * LANES, (half + 1) * LANES)
                            if block == blocks:
                                at = base_e + which * count + 8 * m
                                return rxe[at : at + 8, lanes]
                            at = base + (which * blocks + block) * count + 8 * m
                            return rx[at : at + 8, lanes]

                        both.append(
                            piece(tile, 0)
                            + jnp.where(low_half, piece(tile - 1, 1), piece(tile + 1, 1))
                        )
                    value, product = finish(*both)
                    if beyond:
                        pout[tile, PAD + i0 : PAD + i0 + 8, :] = jnp.where(keep, product, 0.0)
                        dout[tile, PAD + i0 : PAD + i0 + 8, :] = jnp.where(keep, both[1], 0.0)
                        continue
                    if not last_level:
                        pout[tile, PAD + i0 : PAD + i0 + 8, :] = product
                        dout[tile, PAD + i0 : PAD + i0 + 8, :] = both[1]
                    if tile < blocks:
                        vout[i0 : i0 + 8, tile * LANES : (tile + 1) * LANES] = value
                        sums = gather_sums(sums, value, product, both[1])
            base += total
            base_e += 2 * count
        return sums

    all_sums.append(next_level(p1, d1, p2, d2, v2))
    all_sums.append(next_level(p2, d2, p3, d3, v3))
    all_sums.append(next_level(p3, d3, None, None, v4))

    lane = lane_iota(1)
    message = jnp.zeros((1, LANES), F32)

    def whole(x, op):
        return op(op(x, axis=0, keepdims=True), axis=1, keepdims=True)

    for level, sums in enumerate(all_sums):
        for place, (part, op) in enumerate(zip(sums, (jnp.sum, jnp.sum, jnp.max))):
            message = jnp.where(lane == 4 * place + level, whole(part, op), message)

    def exchange(message, buffer, slots, send_sems, recv_sems, index, count, device):
        buffer[...] = message
        slots[index] = message
        copies = []
        for s in range(1, count):
            peer = lax.rem(index + s, count)
            copy = pltpu.make_async_remote_copy(
                src_ref=buffer, dst_ref=slots.at[index],
                send_sem=send_sems.at[s], recv_sem=recv_sems.at[index],
                device_id=device(peer), device_id_type=MESH,
            )
            copy.start()
            copies.append(copy)
        for s in range(1, count):
            peer = lax.rem(index + s, count)
            pltpu.make_async_remote_copy(
                src_ref=buffer, dst_ref=slots.at[peer],
                send_sem=send_sems.at[s], recv_sem=recv_sems.at[peer],
                device_id=device(peer), device_id_type=MESH,
            ).wait_recv()
        added, largest = slots[0], slots[0]
        for i in range(1, count):
            added, largest = added + slots[i], jnp.maximum(largest, slots[i])
        for copy in copies:
            copy.wait_send()
        return jnp.where(lane < 8, added, largest)

    message = exchange(
        message, msg_b, slot_b, b_send, b_recv, my_row, n_rows, lambda peer: (peer, my_col)
    )
    message = exchange(
        message, msg_a, slot_a, a_send, a_recv, my_col, n_cols, lambda peer: (my_row, peer)
    )
    wide = jnp.broadcast_to(message, (8, LANES))
    covers = pltpu.roll(wide, LANES - 4, 1)
    maxima = pltpu.roll(wide, LANES - 8, 1)
    stats[...] = jnp.where(sub == 0, wide / (covers + EPS), maxima)


def copy_out(v1, v2, v3, v4, stats):
    def body(*refs):
        ins, outs, means, maxima, sem = refs[:5], refs[5:9], refs[9], refs[10], refs[11]
        copies = []
        steps = ins[0].shape[0] // 8
        parts = [(0, pl.ds(k * steps, steps)) for k in range(8)]
        parts += [(i, pl.ds(0, ins[i].shape[0])) for i in range(1, 4)]
        for i, at in parts:
            copy = pltpu.make_async_copy(ins[i].at[at, :], outs[i].at[at, :], sem.at[len(copies)])
            copy.start()
            copies.append(copy)
        for i in range(4):
            means[i] = ins[4][0, i]
            maxima[i] = ins[4][1, i]
        for copy in copies:
            copy.wait()

    shapes = [jax.ShapeDtypeStruct(v.shape, F32) for v in (v1, v2, v3, v4)]
    shapes += [jax.ShapeDtypeStruct((4,), F32)] * 2
    return pl.pallas_call(
        body,
        out_shape=shapes,
        in_specs=[pl.BlockSpec(memory_space=pltpu.VMEM)] * 5,
        out_specs=[pl.BlockSpec(memory_space=pl.ANY)] * 4
        + [pl.BlockSpec(memory_space=pltpu.SMEM)] * 2,
        scratch_shapes=[pltpu.SemaphoreType.DMA((11,))],
    )(*[pltpu.with_memory_space_constraint(x, pltpu.VMEM) for x in (v1, v2, v3, v4, stats)])


def per_device(surface_field, land_words):
    rows, cols = surface_field.shape
    n_rows, n_cols = lax.axis_size("rows"), lax.axis_size("cols")
    words = land_words.shape[1]
    chunks = rows // ROW_CHUNK
    blocks = cols // 256
    packed = rows // 8

    def vmem(*shape, dtype=F32):
        return pltpu.VMEM(shape, dtype)

    level = [(rows >> l, cols >> l) for l in range(5)]
    scratch = [
        vmem(rows, cols), vmem(words, rows, dtype=jnp.int32), vmem(rows, LANES, dtype=jnp.int32),
        vmem(2 * HALO, cols), vmem(2 * HALO, LANES, dtype=jnp.int32),
        vmem(2 * packed, LANES), vmem(2 * packed, LANES),
        vmem(2 * packed, LANES), vmem(2 * packed, LANES),
        vmem(4 * HALO, LANES), vmem(4 * HALO, LANES, dtype=jnp.int32),
        vmem(blocks * ROW_CHUNK, 512, dtype=BF16), vmem(blocks * ROW_CHUNK, 256, dtype=BF16),
        vmem(blocks * ROW_CHUNK, 256), vmem(blocks * ROW_CHUNK, 256),
        vmem(blocks * ROW_CHUNK, 512, dtype=BF16), vmem(blocks * ROW_CHUNK, 256, dtype=BF16),
        vmem(blocks * ROW_CHUNK, 256), vmem(blocks * ROW_CHUNK, 256),
        vmem(rows + 2 * HALO, 256, dtype=BF16), vmem(rows + 2 * HALO, LANES, dtype=BF16),
        vmem(rows + 2 * HALO, 256), vmem(rows + 2 * HALO, 256),
        vmem(blocks + 1, rows + 2 * PAD, LANES), vmem(blocks + 1, rows + 2 * PAD, LANES),
        vmem(-(-(rows + 2 * PAD) // LANES) * LANES, LANES),
    ]
    for l in range(1, 4):
        scratch += [vmem(level[l][1] // LANES + 1, level[l][0] + 2 * PAD, LANES)] * 2
    count = level[2][0] + HALO
    inner_blocks = level[2][1] // LANES
    scratch += [
        vmem(2 * inner_blocks * count, 512, dtype=BF16), vmem(2 * count, 256, dtype=BF16),
        vmem(2 * inner_blocks * count, 256), vmem(2 * count, 256),
        vmem(512, 256, dtype=BF16), vmem(256, 256, dtype=BF16),
        vmem(1, LANES), vmem(1, LANES),
        vmem(n_cols, 1, LANES), vmem(n_rows, 1, LANES),
        pltpu.SemaphoreType.DMA((3 + chunks,)),
        pltpu.SemaphoreType.DMA((14,)), pltpu.SemaphoreType.DMA((14,)),
        pltpu.SemaphoreType.DMA((n_cols,)), pltpu.SemaphoreType.DMA((n_cols,)),
        pltpu.SemaphoreType.DMA((n_rows,)), pltpu.SemaphoreType.DMA((n_rows,)),
    ]
    out_shape = [pltpu.VMEM(level[l], F32) for l in range(1, 5)]
    out_shape.append(pltpu.VMEM((8, LANES), F32))
    v1, v2, v3, v4, stats = pl.pallas_call(
        kernel,
        out_shape=out_shape,
        in_specs=[pl.BlockSpec(memory_space=pl.ANY)] * 2,
        out_specs=[pl.BlockSpec(memory_space=pltpu.VMEM)] * 5,
        scratch_shapes=scratch,
        compiler_params=pltpu.CompilerParams(
            collective_id=0, has_side_effects=True, vmem_limit_bytes=48 * 1024 * 1024
        ),
    )(
        pltpu.with_memory_space_constraint(surface_field, pltpu.HBM),
        pltpu.with_memory_space_constraint(land_words.T, pltpu.HBM),
    )
    return copy_out(v1, v2, v3, v4, stats)


def solution(mesh):
    spec = P("rows", "cols")
    return jax.shard_map(
        per_device, mesh=mesh, in_specs=(spec, spec),
        out_specs=(spec, spec, spec, spec, P(), P()), check_vma=False,
    )
```

```python
import math

import jax
import jax.numpy as jnp
from jax import lax
from jax.experimental import pallas as pl
from jax.experimental.pallas import tpu as pltpu
from jax.sharding import PartitionSpec as P

MESH = pl.DeviceIdType.MESH
F32 = jnp.float32
BF16 = jnp.bfloat16
HALO = 16
PAD = 24
LANES = 128
ROW_CHUNK = 64
FLOOR = 0.05
EPS = 1e-06


def lane_iota(rows, dtype=jnp.int32):
    return lax.broadcasted_iota(dtype, (rows, LANES), 1)


def tap_weight(offset):
    inner = jnp.logical_or(offset == 1, offset == 2)
    outer = jnp.logical_or(offset == 0, offset == 3)
    return jnp.where(inner, 0.375, jnp.where(outer, 0.125, 0.0))


def build_tables(band, edge):
    k = lax.broadcasted_iota(jnp.int32, (256, 256), 0)
    n = lax.broadcasted_iota(jnp.int32, (256, 256), 1)
    own = tap_weight(k - (2 * n - 1))
    spill = jnp.logical_or(
        jnp.logical_and(n == 128, k == 255), jnp.logical_and(n == 255, k == 0)
    )
    table = jnp.where(n < 128, own, jnp.where(spill, 0.125, 0.0))
    band[0:256, :] = table.astype(BF16)
    band[256:512, :] = table.astype(BF16)
    k = lax.broadcasted_iota(jnp.int32, (128, 256), 0)
    n = lax.broadcasted_iota(jnp.int32, (128, 256), 1)
    right = jnp.where(k < 64, tap_weight(k - (2 * n - 1)), 0.0)
    left = jnp.where(k >= 64, tap_weight(k - (2 * n - 129)), 0.0)
    spill = jnp.logical_or(
        jnp.logical_and(n == 128, k == 127), jnp.logical_and(n == 255, k == 0)
    )
    table = jnp.where(
        n < 64, right, jnp.where(n < 128, left, jnp.where(spill, 0.125, 0.0))
    ).astype(BF16)
    edge[0:128, :] = table
    edge[128:256, :] = table


def pieces(x):
    high = x.astype(BF16)
    low = (x - high.astype(F32)).astype(BF16)
    return high, low


def land_of(words, tile):
    rows = words.shape[0]
    lane = lane_iota(rows)
    picked = jnp.take_along_axis(
        words, 4 * tile + lane // 32, axis=1, mode="promise_in_bounds"
    )
    return jnp.left_shift(picked, 31 - lane % 32) < 0


def dot(a, b):
    return jnp.dot(a, b, preferred_element_type=F32)


def mask_step(field_tile, words, rows, s_num, s_den, tiles):
    for tile in range(tiles):
        land = land_of(words, tile)
        masked = jnp.where(land, field_tile(tile), 0.0)
        at = (tile // 2) * rows
        half = (tile % 2) * LANES
        high, low = pieces(masked)
        s_num[at : at + rows, half : half + LANES] = high
        s_num[at : at + rows, 256 + half : 256 + half + LANES] = low
        s_den[at : at + rows, half : half + LANES] = jnp.where(land, 1.0, 0.0).astype(BF16)


def across_step(rows, s_num, s_den, r_num, r_den, band, tiles, store):
    blocks = tiles // 2
    r_num[0 : blocks * rows, :] = dot(s_num[0 : blocks * rows, :], band[...])
    r_den[0 : blocks * rows, :] = dot(s_den[0 : blocks * rows, :], band[0:256, :])
    low_half = lane_iota(rows) < 64
    for which, ref in ((0, r_num), (1, r_den)):
        def spill(block):
            if block < 0 or block >= blocks:
                return jnp.zeros((rows, LANES), F32)
            return ref[block * rows : (block + 1) * rows, LANES : 2 * LANES]

        for block in range(blocks):
            own = ref[block * rows : (block + 1) * rows, 0:LANES]
            store(which, block, own + jnp.where(low_half, spill(block - 1), spill(block + 1)))
        store(which, blocks, jnp.where(low_half, spill(blocks - 1), spill(0)))


def first_across(field_tile, words, rows, s_num, s_den, r_num, r_den, band, tiles, store):
    mask_step(field_tile, words, rows, s_num, s_den, tiles)
    across_step(rows, s_num, s_den, r_num, r_den, band, tiles, store)


def kernel(
    field_hbm, words_hbm,
    v1, v2, v3, v4, stats,
    fld, wrd_cols, wrd, fhal, whal, out_left, out_right, in_left, in_right, cornf, cornw,
    s_num, s_den, r_num, r_den, s_num2, s_den2, r_num2, r_den2, se_num, se_den, re_num, re_den,
    hn, hd, cosb, p1, d1, p2, d2, p3, d3,
    sx, sxe, rx, rxe, band, edge, msg_a, msg_b, slot_a, slot_b,
    load_sem, send_sem, recv_sem, a_send, a_recv, b_send, b_recv,
    beside_sem, far_sem,
):
    n_rows, n_cols = lax.axis_size("rows"), lax.axis_size("cols")
    my_row, my_col = lax.axis_index("rows"), lax.axis_index("cols")
    rows, cols = fld.shape
    tiles = cols // LANES
    up, down = lax.rem(my_row + n_rows - 1, n_rows), lax.rem(my_row + 1, n_rows)
    left, right = lax.rem(my_col + n_cols - 1, n_cols), lax.rem(my_col + 1, n_cols)

    barrier = pltpu.get_barrier_semaphore()
    half_rows = n_rows // 2
    half_start = my_row // half_rows * half_rows
    far_row = lax.rem(my_row + half_rows, n_rows)
    peers = [(my_row, lax.rem(my_col + s, n_cols)) for s in range(1, n_cols)]
    peers += [
        (half_start + lax.rem(my_row - half_start + s, half_rows), my_col)
        for s in range(1, half_rows)
    ]
    peers += [(far_row, my_col), (up, my_col), (down, my_col)]
    for peer in peers:
        pl.semaphore_signal(barrier, inc=1, device_id=peer, device_id_type=MESH)

    loads = []

    def load(src, dst):
        copy = pltpu.make_async_copy(src, dst, load_sem.at[len(loads)])
        copy.start()
        loads.append(copy)
        return copy

    load_words = load(words_hbm, wrd_cols)
    load_strips = [
        load(field_hbm.at[:, 0:LANES], fld.at[:, 0:LANES]),
        load(field_hbm.at[:, cols - LANES : cols], fld.at[:, cols - LANES : cols]),
    ]
    chunks = rows // ROW_CHUNK
    order = [0, chunks - 1] + list(range(1, chunks - 1))
    load_chunk = {}
    for c in order:
        at = pl.ds(c * ROW_CHUNK, ROW_CHUNK)
        load_chunk[c] = load(
            field_hbm.at[at, LANES : cols - LANES], fld.at[at, LANES : cols - LANES]
        )

    build_tables(band, edge)
    for ref in (hn, hd, p1, d1, p2, d2, p3, d3):
        spare = PAD - HALO if ref.shape[1] == rows + 2 * PAD else HALO
        zeros = jnp.zeros((ref.shape[0], spare, LANES), F32)
        ref[:, 0:spare, :] = zeros
        ref[:, ref.shape[1] - spare :, :] = zeros

    sub = lax.broadcasted_iota(jnp.int32, (8, LANES), 0)
    global_row = my_row * rows - PAD + sub * LANES + lane_iota(8)
    latitude = ((global_row.astype(F32) + 0.5) / (rows * n_rows) - 0.5) * math.pi
    on_globe = jnp.logical_and(global_row >= 0, global_row < rows * n_rows)
    cosines = jnp.where(on_globe, jnp.cos(latitude) * 0.125, 0.0)
    for q in range(cosb.shape[0] // LANES):
        row = jnp.broadcast_to(cosines[q : q + 1, :], (LANES, LANES))
        cosb[q * LANES : (q + 1) * LANES, :] = jnp.transpose(row)

    load_words.wait()
    copies_of = LANES // wrd_cols.shape[0]
    for q in range(rows // LANES):
        at = slice(q * LANES, (q + 1) * LANES)
        wrd[at, :] = jnp.transpose(jnp.concatenate([wrd_cols[:, at]] * copies_of, axis=0))

    for copy in load_strips:
        copy.wait()
    packed = rows // 8
    lane = lane_iota(packed)
    for out, tile, shift in ((out_left, 0, 0), (out_right, tiles - 1, HALO)):
        field_part = jnp.zeros((packed, LANES), F32)
        land_part = jnp.zeros((packed, LANES), F32)
        for g in range(8):
            at = slice(g * packed, (g + 1) * packed)
            values = fld[at, tile * LANES : (tile + 1) * LANES]
            land = jnp.where(land_of(wrd[at, :], tile), 1.0, 0.0)
            turn = (HALO * g + shift) % LANES
            if turn:
                values, land = pltpu.roll(values, turn, 1), pltpu.roll(land, turn, 1)
            here = lane // HALO == g
            field_part = jnp.where(here, values, field_part)
            land_part = jnp.where(here, land, land_part)
        out[0:packed, :] = field_part
        out[packed : 2 * packed, :] = land_part
    load_chunk[0].wait()
    if chunks > 1:
        load_chunk[chunks - 1].wait()

    pl.semaphore_wait(barrier, len(peers))

    sends = []

    def send(src, dst, row, col):
        i = len(sends)
        copy = pltpu.make_async_remote_copy(
            src_ref=src, dst_ref=dst, send_sem=send_sem.at[i], recv_sem=recv_sem.at[i],
            device_id=(row, col), device_id_type=MESH,
        )
        copy.start()
        sends.append(copy)

    top, bottom = slice(0, HALO), slice(rows - HALO, rows)
    last_tile = slice(cols - LANES, cols)
    send(out_left, in_right, my_row, left)
    send(out_right, in_left, my_row, right)
    send(fld.at[top, :], fhal.at[HALO : 2 * HALO, :], up, my_col)
    send(fld.at[bottom, :], fhal.at[0:HALO, :], down, my_col)
    send(wrd.at[top, :], whal.at[HALO : 2 * HALO, :], up, my_col)
    send(wrd.at[bottom, :], whal.at[0:HALO, :], down, my_col)
    for column in (left, right):
        pl.semaphore_signal(
            beside_sem, inc=1, device_id=(my_row, column), device_id_type=MESH
        )
    pl.semaphore_signal(far_sem, inc=1, device_id=(far_row, my_col), device_id_type=MESH)

    for c in order[2:]:
        load_chunk[c].wait()

    sets = ((s_num, s_den, r_num, r_den), (s_num2, s_den2, r_num2, r_den2))

    def own_mask(at, which):
        def field_tile(tile):
            return fld[pl.ds(at, ROW_CHUNK), tile * LANES : (tile + 1) * LANES]

        mask_step(
            field_tile, wrd[pl.ds(at, ROW_CHUNK), :], ROW_CHUNK, *sets[which][0:2], tiles
        )

    def own_across(at, which):
        def store(which, tile, value):
            ref = (hn, hd)[which]
            ref[tile, pl.ds(PAD + at, ROW_CHUNK), :] = value

        across_step(ROW_CHUNK, *sets[which], band, tiles, store)

    def own_chunks(first, last):
        own_mask(first * ROW_CHUNK, first % 2)
        for c in range(first, last):
            if c + 1 < last:
                own_mask((c + 1) * ROW_CHUNK, (c + 1) % 2)
            own_across(c * ROW_CHUNK, c % 2)

    own_chunks(0, chunks // 2)

    pl.semaphore_wait(beside_sem, 2)
    send(fld.at[bottom, last_tile], cornf.at[0 * HALO : 1 * HALO, :], down, right)
    send(fld.at[bottom, 0:LANES], cornf.at[1 * HALO : 2 * HALO, :], down, left)
    send(fld.at[top, last_tile], cornf.at[2 * HALO : 3 * HALO, :], up, right)
    send(fld.at[top, 0:LANES], cornf.at[3 * HALO : 4 * HALO, :], up, left)
    send(wrd.at[bottom, :], cornw.at[0 * HALO : 1 * HALO, :], down, right)
    send(wrd.at[bottom, :], cornw.at[1 * HALO : 2 * HALO, :], down, left)
    send(wrd.at[top, :], cornw.at[2 * HALO : 3 * HALO, :], up, right)
    send(wrd.at[top, :], cornw.at[3 * HALO : 4 * HALO, :], up, left)

    own_chunks(chunks // 2, chunks)

    inside_top, inside_bottom = my_row > 0, my_row < n_rows - 1
    out_rows, out_tiles = rows // 2, tiles // 2

    def finish(num, den):
        value = num / jnp.maximum(den, FLOOR)
        return value, den * value

    zero_sums = (
        jnp.zeros((8, LANES), F32), jnp.zeros((8, LANES), F32), jnp.full((8, LANES), -jnp.inf, F32)
    )

    def gather_sums(sums, value, product, cover):
        return (sums[0] + product, sums[1] + cover, jnp.maximum(sums[2], value))

    def level_one_rows(i0, tile, cosine):
        result = []
        for ref in (hn, hd):
            taps = [ref[tile, pl.ds(PAD + 2 * i0 - 1 + a, 8, stride=2), :] for a in range(4)]
            taps = [t * c for t, c in zip(taps, cosine)]
            result.append((taps[0] + taps[3]) + (taps[1] + taps[2]))
        return result

    def cosine_of(i0):
        taps = [cosb[pl.ds(PAD + 2 * i0 - 1 + a, 8, stride=2), :] for a in range(4)]
        return [taps[0], 3.0 * taps[1], 3.0 * taps[2], taps[3]]

    def level_one_own(i0, which_tiles, sums):
        cosine = cosine_of(i0)
        for tile in which_tiles:
            num, den = level_one_rows(i0, tile, cosine)
            value, product = finish(num, den)
            p1[tile, pl.ds(PAD + i0, 8), :] = product
            d1[tile, pl.ds(PAD + i0, 8), :] = den
            if tile < out_tiles:
                v1[pl.ds(i0, 8), tile * LANES : (tile + 1) * LANES] = value
                sums = gather_sums(sums, value, product, den)
        return sums

    def level_one_inner(which_tiles, sums):
        def pair(c, sums):
            i0 = pl.multiple_of(8 + c * 16, 8)
            sums = level_one_own(i0, which_tiles, sums)
            return level_one_own(i0 + 8, which_tiles, sums)

        return lax.fori_loop(0, out_rows // 16 - 1, pair, sums)

    def level_one_beyond(i0, keep):
        cosine = cosine_of(i0)
        for tile in range(out_tiles + 1):
            num, den = level_one_rows(i0, tile, cosine)
            value, product = finish(num, den)
            p1[tile, PAD + i0 : PAD + i0 + 8, :] = jnp.where(keep, product, 0.0)
            d1[tile, PAD + i0 : PAD + i0 + 8, :] = jnp.where(keep, den, 0.0)

    sums_one = level_one_inner(range(1, out_tiles - 1), zero_sums)

    for copy in sends[0:2]:
        copy.wait()

    def edge_store(at, count, field_value, land_value):
        high, low = pieces(field_value * land_value)
        se_num[at : at + count, 0:LANES] = high
        se_num[at : at + count, LANES : 2 * LANES] = low
        se_den[at : at + count, :] = land_value.astype(BF16)

    def edge_dot(at, count):
        here = slice(at, at + count)
        re_num[here, :] = dot(se_num[here, :], edge[...])
        re_den[here, :] = dot(se_den[here, :], edge[0:128, :])

    def merge_edge(src, dst, count):
        low_half = lane_iota(count) < 64
        for result, ref in ((re_num, hn), (re_den, hd)):
            spill = result[src : src + count, LANES : 2 * LANES]
            here = slice(dst, dst + count)
            last = out_tiles - 1
            ref[0, here, :] = ref[0, here, :] + jnp.where(low_half, spill, 0.0)
            ref[last, here, :] = ref[last, here, :] + jnp.where(low_half, 0.0, spill)
            ref[out_tiles, here, :] = (
                ref[out_tiles, here, :] + result[src : src + count, 0:LANES]
            )

    for g in range(8):
        parts = []
        for base in (0, packed):
            from_right = in_right[base : base + packed, :]
            from_left = in_left[base : base + packed, :]
            turn = (LANES - HALO * g) % LANES
            if turn:
                from_right = pltpu.roll(from_right, turn, 1)
            turn = (LANES - HALO - HALO * g) % LANES
            if turn:
                from_left = pltpu.roll(from_left, turn, 1)
            parts.append(
                jnp.where(
                    lane < HALO, from_right, jnp.where(lane >= LANES - HALO, from_left, 0.0)
                )
            )
        edge_store(g * packed, packed, parts[0], parts[1])
    edge_dot(0, rows)
    merge_edge(0, PAD, rows)
    sums_one = level_one_inner((0, out_tiles - 1, out_tiles), sums_one)

    def row_groups(ref):
        return [(i0, i0 + 8) for i0 in range(0, ref.shape[0], 16)]

    def next_level(pin, din, pout, dout, vout):
        out_rows, out_cols = vout.shape
        blocks = out_cols // LANES
        last_level = pout is None
        next_free = [0, 0]
        low_half = lane_iota(8) < 64

        def down_rows(ref, i0, tile):
            taps = [ref[tile, pl.ds(PAD + 2 * i0 - 1 + a, 8, stride=2), :] for a in range(4)]
            return 0.125 * (taps[0] + taps[3]) + 0.375 * (taps[1] + taps[2])

        def run(part, sums):
            base, base_e = next_free
            count = 16 * len(part)
            for g, pair in enumerate(part):
                for which, ref in ((0, pin), (1, din)):
                    for tile in range(2 * blocks + 1):
                        value = jnp.concatenate(
                            [down_rows(ref, i0, tile) for i0 in pair], axis=0
                        )
                        high, low = pieces(value)
                        if tile < 2 * blocks:
                            at = base + (which * blocks + tile // 2) * count + 16 * g
                            half = (tile % 2) * LANES
                            sx[at : at + 16, half : half + LANES] = high
                            sx[at : at + 16, 256 + half : 256 + half + LANES] = low
                        else:
                            at = base_e + which * count + 16 * g
                            sxe[at : at + 16, 0:LANES] = high
                            sxe[at : at + 16, LANES : 2 * LANES] = low
            total = 2 * blocks * count
            rx[base : base + total, :] = dot(sx[base : base + total, :], band[...])
            rxe[base_e : base_e + 2 * count, :] = dot(
                sxe[base_e : base_e + 2 * count, :], edge[...]
            )
            starts = [i0 for pair in part for i0 in pair]
            for m, i0 in enumerate(starts):
                beyond = i0 < 0 or i0 >= out_rows
                keep = inside_top if i0 < 0 else inside_bottom
                for tile in range(blocks + (0 if last_level else 1)):
                    both = []
                    for which in range(2):
                        def piece(block, half, which=which):
                            block = block % (blocks + 1)
                            lanes = slice(half * LANES, (half + 1) * LANES)
                            if block == blocks:
                                at = base_e + which * count + 8 * m
                                return rxe[at : at + 8, lanes]
                            at = base + (which * blocks + block) * count + 8 * m
                            return rx[at : at + 8, lanes]

                        both.append(
                            piece(tile, 0)
                            + jnp.where(low_half, piece(tile - 1, 1), piece(tile + 1, 1))
                        )
                    value, product = finish(*both)
                    if beyond:
                        pout[tile, PAD + i0 : PAD + i0 + 8, :] = jnp.where(keep, product, 0.0)
                        dout[tile, PAD + i0 : PAD + i0 + 8, :] = jnp.where(keep, both[1], 0.0)
                        continue
                    if not last_level:
                        pout[tile, PAD + i0 : PAD + i0 + 8, :] = product
                        dout[tile, PAD + i0 : PAD + i0 + 8, :] = both[1]
                    if tile < blocks:
                        vout[i0 : i0 + 8, tile * LANES : (tile + 1) * LANES] = value
                        sums = gather_sums(sums, value, product, both[1])
            next_free[0], next_free[1] = base + total, base_e + 2 * count
            return sums

        return run

    two = next_level(p1, d1, p2, d2, v2)
    groups_two = row_groups(v2)
    middle = groups_two[1:-1]
    sums_two = zero_sums
    for i in range(0, len(middle), 3):
        sums_two = two(middle[i : i + 3], sums_two)

    for copy in sends[2:6]:
        copy.wait()

    def halo_store(which, tile, value):
        ref = (hn, hd)[which]
        ref[tile, PAD - HALO : PAD, :] = value[0:HALO, :]
        ref[tile, PAD + rows : PAD + rows + HALO, :] = value[HALO : 2 * HALO, :]

    first_across(
        lambda tile: fhal[:, tile * LANES : (tile + 1) * LANES], whal[...], 2 * HALO,
        s_num, s_den, r_num, r_den, band, tiles, halo_store,
    )
    for copy in sends[6:]:
        copy.wait()
    lane16 = lane_iota(HALO)
    for side in range(2):
        l_at = slice(2 * side * HALO, (2 * side + 1) * HALO)
        r_at = slice((2 * side + 1) * HALO, (2 * side + 2) * HALO)
        is_right, is_left = lane16 < HALO, lane16 >= LANES - HALO
        value = jnp.where(is_right, cornf[r_at, :], jnp.where(is_left, cornf[l_at, :], 0.0))
        land_r = jnp.where(land_of(cornw[r_at, :], 0), 1.0, 0.0)
        land_l = jnp.where(land_of(cornw[l_at, :], tiles - 1), 1.0, 0.0)
        land = jnp.where(is_right, land_r, jnp.where(is_left, land_l, 0.0))
        edge_store(rows + side * HALO, HALO, value, land)
    edge_dot(rows, 2 * HALO)
    merge_edge(rows, PAD - HALO, HALO)
    merge_edge(rows + HALO, PAD + rows, HALO)
    for i0 in (0, out_rows - 8):
        sums_one = level_one_own(i0, range(out_tiles + 1), sums_one)
    level_one_beyond(-8, inside_top)
    level_one_beyond(out_rows, inside_bottom)
    sums_two = two([groups_two[0], groups_two[-1], (-8, v2.shape[0])], sums_two)
    groups_three = row_groups(v3) + [(-8, v3.shape[0])]
    sums_three = next_level(p2, d2, p3, d3, v3)(groups_three, zero_sums)
    sums_four = next_level(p3, d3, None, None, v4)(row_groups(v4), zero_sums)
    all_sums = [sums_one, sums_two, sums_three, sums_four]

    lane = lane_iota(1)
    message = jnp.zeros((1, LANES), F32)

    def whole(x, op):
        return op(op(x, axis=0, keepdims=True), axis=1, keepdims=True)

    for level, sums in enumerate(all_sums):
        for place, (part, op) in enumerate(zip(sums, (jnp.sum, jnp.sum, jnp.max))):
            message = jnp.where(lane == 4 * place + level, whole(part, op), message)

    def exchange(message, buffer, slots, send_sems, recv_sems, index, count, device):
        buffer[...] = message
        slots[index] = message
        copies = []
        for s in range(1, count):
            peer = lax.rem(index + s, count)
            copy = pltpu.make_async_remote_copy(
                src_ref=buffer, dst_ref=slots.at[index],
                send_sem=send_sems.at[s], recv_sem=recv_sems.at[index],
                device_id=device(peer), device_id_type=MESH,
            )
            copy.start()
            copies.append(copy)
        for s in range(1, count):
            peer = lax.rem(index + s, count)
            pltpu.make_async_remote_copy(
                src_ref=buffer, dst_ref=slots.at[peer],
                send_sem=send_sems.at[s], recv_sem=recv_sems.at[peer],
                device_id=device(peer), device_id_type=MESH,
            ).wait_recv()
        added, largest = slots[0], slots[0]
        for i in range(1, count):
            added, largest = added + slots[i], jnp.maximum(largest, slots[i])
        for copy in copies:
            copy.wait_send()
        return jnp.where(lane < 8, added, largest)

    pl.semaphore_wait(far_sem, 1)
    message = exchange(
        message, msg_b, slot_b, b_send, b_recv, my_row, n_rows, lambda peer: (peer, my_col)
    )
    message = exchange(
        message, msg_a, slot_a, a_send, a_recv, my_col, n_cols, lambda peer: (my_row, peer)
    )
    wide = jnp.broadcast_to(message, (8, LANES))
    covers = pltpu.roll(wide, LANES - 4, 1)
    maxima = pltpu.roll(wide, LANES - 8, 1)
    stats[...] = jnp.where(sub == 0, wide / (covers + EPS), maxima)


def copy_out(v1, v2, v3, v4, stats):
    def body(*refs):
        ins, outs, small_outs = refs[:5], refs[5:9], refs[9:11]
        small, sem = refs[11:13], refs[13]
        copies = []
        steps = ins[0].shape[0] // 8
        parts = [(0, pl.ds(k * steps, steps)) for k in range(8)]
        parts += [(i, pl.ds(0, ins[i].shape[0])) for i in range(1, 4)]
        for i, at in parts:
            copy = pltpu.make_async_copy(ins[i].at[at, :], outs[i].at[at, :], sem.at[len(copies)])
            copy.start()
            copies.append(copy)
        for which in range(2):
            for i in range(4):
                small[which][i] = ins[4][which, i]
            copy = pltpu.make_async_copy(small[which], small_outs[which], sem.at[len(copies)])
            copy.start()
            copies.append(copy)
        for copy in copies:
            copy.wait()

    shapes = [jax.ShapeDtypeStruct(v.shape, F32) for v in (v1, v2, v3, v4)]
    shapes += [jax.ShapeDtypeStruct((4,), F32)] * 2
    return pl.pallas_call(
        body,
        out_shape=shapes,
        in_specs=[pl.BlockSpec(memory_space=pltpu.VMEM)] * 5,
        out_specs=[pl.BlockSpec(memory_space=pl.ANY)] * 6,
        scratch_shapes=[pltpu.SMEM((4,), F32)] * 2 + [pltpu.SemaphoreType.DMA((13,))],
    )(*[pltpu.with_memory_space_constraint(x, pltpu.VMEM) for x in (v1, v2, v3, v4, stats)])


def per_device(surface_field, land_words):
    rows, cols = surface_field.shape
    n_rows, n_cols = lax.axis_size("rows"), lax.axis_size("cols")
    words = land_words.shape[1]
    chunks = rows // ROW_CHUNK
    blocks = cols // 256
    packed = rows // 8

    def vmem(*shape, dtype=F32):
        return pltpu.VMEM(shape, dtype)

    level = [(rows >> l, cols >> l) for l in range(5)]
    scratch = [
        vmem(rows, cols), vmem(words, rows, dtype=jnp.int32), vmem(rows, LANES, dtype=jnp.int32),
        vmem(2 * HALO, cols), vmem(2 * HALO, LANES, dtype=jnp.int32),
        vmem(2 * packed, LANES), vmem(2 * packed, LANES),
        vmem(2 * packed, LANES), vmem(2 * packed, LANES),
        vmem(4 * HALO, LANES), vmem(4 * HALO, LANES, dtype=jnp.int32),
        vmem(blocks * ROW_CHUNK, 512, dtype=BF16), vmem(blocks * ROW_CHUNK, 256, dtype=BF16),
        vmem(blocks * ROW_CHUNK, 256), vmem(blocks * ROW_CHUNK, 256),
        vmem(blocks * ROW_CHUNK, 512, dtype=BF16), vmem(blocks * ROW_CHUNK, 256, dtype=BF16),
        vmem(blocks * ROW_CHUNK, 256), vmem(blocks * ROW_CHUNK, 256),
        vmem(rows + 2 * HALO, 256, dtype=BF16), vmem(rows + 2 * HALO, LANES, dtype=BF16),
        vmem(rows + 2 * HALO, 256), vmem(rows + 2 * HALO, 256),
        vmem(blocks + 1, rows + 2 * PAD, LANES), vmem(blocks + 1, rows + 2 * PAD, LANES),
        vmem(-(-(rows + 2 * PAD) // LANES) * LANES, LANES),
    ]
    for l in range(1, 4):
        scratch += [vmem(level[l][1] // LANES + 1, level[l][0] + 2 * PAD, LANES)] * 2
    count = level[2][0] + HALO
    inner_blocks = level[2][1] // LANES
    scratch += [
        vmem(2 * inner_blocks * count, 512, dtype=BF16), vmem(2 * count, 256, dtype=BF16),
        vmem(2 * inner_blocks * count, 256), vmem(2 * count, 256),
        vmem(512, 256, dtype=BF16), vmem(256, 256, dtype=BF16),
        vmem(1, LANES), vmem(1, LANES),
        vmem(n_cols, 1, LANES), vmem(n_rows, 1, LANES),
        pltpu.SemaphoreType.DMA((3 + chunks,)),
        pltpu.SemaphoreType.DMA((14,)), pltpu.SemaphoreType.DMA((14,)),
        pltpu.SemaphoreType.DMA((n_cols,)), pltpu.SemaphoreType.DMA((n_cols,)),
        pltpu.SemaphoreType.DMA((n_rows,)), pltpu.SemaphoreType.DMA((n_rows,)),
        pltpu.SemaphoreType.REGULAR, pltpu.SemaphoreType.REGULAR,
    ]
    out_shape = [pltpu.VMEM(level[l], F32) for l in range(1, 5)]
    out_shape.append(pltpu.VMEM((8, LANES), F32))
    v1, v2, v3, v4, stats = pl.pallas_call(
        kernel,
        out_shape=out_shape,
        in_specs=[pl.BlockSpec(memory_space=pl.ANY)] * 2,
        out_specs=[pl.BlockSpec(memory_space=pltpu.VMEM)] * 5,
        scratch_shapes=scratch,
        compiler_params=pltpu.CompilerParams(
            collective_id=0, has_side_effects=True, vmem_limit_bytes=48 * 1024 * 1024
        ),
    )(
        pltpu.with_memory_space_constraint(surface_field, pltpu.HBM),
        pltpu.with_memory_space_constraint(land_words.T, pltpu.HBM),
    )
    return copy_out(v1, v2, v3, v4, stats)


def solution(mesh):
    spec = P("rows", "cols")
    return jax.shard_map(
        per_device, mesh=mesh, in_specs=(spec, spec),
        out_specs=(spec, spec, spec, spec, P(), P()), check_vma=False,
    )
```

```python
import math

import jax
import jax.numpy as jnp
from jax import lax
from jax.experimental import pallas as pl
from jax.experimental.pallas import tpu as pltpu
from jax.sharding import PartitionSpec as P

MESH = pl.DeviceIdType.MESH
F32 = jnp.float32
BF16 = jnp.bfloat16
HALO = 16
PAD = 24
LANES = 128
ROW_CHUNK = 64
FLOOR = 0.05
EPS = 1e-06


def lane_iota(rows, dtype=jnp.int32):
    return lax.broadcasted_iota(dtype, (rows, LANES), 1)


def tap_weight(offset):
    inner = jnp.logical_or(offset == 1, offset == 2)
    outer = jnp.logical_or(offset == 0, offset == 3)
    return jnp.where(inner, 0.375, jnp.where(outer, 0.125, 0.0))


def build_tables(band, edge):
    k = lax.broadcasted_iota(jnp.int32, (256, 256), 0)
    n = lax.broadcasted_iota(jnp.int32, (256, 256), 1)
    own = tap_weight(k - (2 * n - 1))
    spill = jnp.logical_or(
        jnp.logical_and(n == 128, k == 255), jnp.logical_and(n == 255, k == 0)
    )
    table = jnp.where(n < 128, own, jnp.where(spill, 0.125, 0.0))
    band[0:256, :] = table.astype(BF16)
    band[256:512, :] = table.astype(BF16)
    k = lax.broadcasted_iota(jnp.int32, (128, 256), 0)
    n = lax.broadcasted_iota(jnp.int32, (128, 256), 1)
    right = jnp.where(k < 64, tap_weight(k - (2 * n - 1)), 0.0)
    left = jnp.where(k >= 64, tap_weight(k - (2 * n - 129)), 0.0)
    spill = jnp.logical_or(
        jnp.logical_and(n == 128, k == 127), jnp.logical_and(n == 255, k == 0)
    )
    table = jnp.where(
        n < 64, right, jnp.where(n < 128, left, jnp.where(spill, 0.125, 0.0))
    ).astype(BF16)
    edge[0:128, :] = table
    edge[128:256, :] = table


def pieces(x):
    high = x.astype(BF16)
    low = (x - high.astype(F32)).astype(BF16)
    return high, low


def land_of(words, tile):
    rows = words.shape[0]
    lane = lane_iota(rows)
    picked = jnp.take_along_axis(
        words, 4 * tile + lane // 32, axis=1, mode="promise_in_bounds"
    )
    return jnp.left_shift(picked, 31 - lane % 32) < 0


def dot(a, b):
    return jnp.dot(a, b, preferred_element_type=F32)


def mask_step(field_tile, words, rows, s_num, s_den, tiles):
    for tile in range(tiles):
        land = land_of(words, tile)
        masked = jnp.where(land, field_tile(tile), 0.0)
        at = (tile // 2) * rows
        half = (tile % 2) * LANES
        high, low = pieces(masked)
        s_num[at : at + rows, half : half + LANES] = high
        s_num[at : at + rows, 256 + half : 256 + half + LANES] = low
        s_den[at : at + rows, half : half + LANES] = jnp.where(land, 1.0, 0.0).astype(BF16)


def across_step(rows, s_num, s_den, r_num, r_den, band, tiles, store):
    blocks = tiles // 2
    r_num[0 : blocks * rows, :] = dot(s_num[0 : blocks * rows, :], band[...])
    r_den[0 : blocks * rows, :] = dot(s_den[0 : blocks * rows, :], band[0:256, :])
    low_half = lane_iota(rows) < 64
    for which, ref in ((0, r_num), (1, r_den)):
        def spill(block):
            if block < 0 or block >= blocks:
                return jnp.zeros((rows, LANES), F32)
            return ref[block * rows : (block + 1) * rows, LANES : 2 * LANES]

        for block in range(blocks):
            own = ref[block * rows : (block + 1) * rows, 0:LANES]
            store(which, block, own + jnp.where(low_half, spill(block - 1), spill(block + 1)))
        store(which, blocks, jnp.where(low_half, spill(blocks - 1), spill(0)))


def first_across(field_tile, words, rows, s_num, s_den, r_num, r_den, band, tiles, store):
    mask_step(field_tile, words, rows, s_num, s_den, tiles)
    across_step(rows, s_num, s_den, r_num, r_den, band, tiles, store)


def kernel(
    field_hbm, words_hbm,
    v1, v2, v3, v4, stats,
    fld, wrd_cols, wrd, fhal, whal, out_left, out_right, in_left, in_right, cornf, cornw,
    s_num, s_den, r_num, r_den, s_num2, s_den2, r_num2, r_den2, se_num, se_den, re_num, re_den,
    hn, hd, cosb, p1, d1, p2, d2, p3, d3,
    sx, sxe, rx, rxe, band, edge, msg_a, msg_b, slot_a, slot_b,
    load_sem, send_sem, recv_sem, a_send, a_recv, b_send, b_recv,
    beside_sem, far_sem,
):
    n_rows, n_cols = lax.axis_size("rows"), lax.axis_size("cols")
    my_row, my_col = lax.axis_index("rows"), lax.axis_index("cols")
    rows, cols = fld.shape
    tiles = cols // LANES
    up, down = lax.rem(my_row + n_rows - 1, n_rows), lax.rem(my_row + 1, n_rows)
    left, right = lax.rem(my_col + n_cols - 1, n_cols), lax.rem(my_col + 1, n_cols)

    barrier = pltpu.get_barrier_semaphore()
    half_rows = n_rows // 2
    half_start = my_row // half_rows * half_rows
    far_row = lax.rem(my_row + half_rows, n_rows)
    peers = [(up, my_col), (down, my_col), (far_row, my_col)]
    peers += [
        (my_row, lax.rem(my_col + s, n_cols))
        for s in sorted(range(1, n_cols), key=lambda s: min(s, n_cols - s))
    ]
    peers += [
        (half_start + lax.rem(my_row - half_start + s, half_rows), my_col)
        for s in range(1, half_rows)
    ]
    for peer in peers:
        pl.semaphore_signal(barrier, inc=1, device_id=peer, device_id_type=MESH)

    loads = []

    def load(src, dst):
        copy = pltpu.make_async_copy(src, dst, load_sem.at[len(loads)])
        copy.start()
        loads.append(copy)
        return copy

    load_words = load(words_hbm, wrd_cols)
    load_strips = [
        load(field_hbm.at[:, 0:LANES], fld.at[:, 0:LANES]),
        load(field_hbm.at[:, cols - LANES : cols], fld.at[:, cols - LANES : cols]),
    ]
    chunks = rows // ROW_CHUNK
    order = [0, chunks - 1] + list(range(1, chunks - 1))
    load_chunk = {}
    for c in order:
        at = pl.ds(c * ROW_CHUNK, ROW_CHUNK)
        load_chunk[c] = load(
            field_hbm.at[at, LANES : cols - LANES], fld.at[at, LANES : cols - LANES]
        )

    build_tables(band, edge)
    for ref in (hn, hd, p1, d1, p2, d2, p3, d3):
        spare = PAD - HALO if ref.shape[1] == rows + 2 * PAD else HALO
        zeros = jnp.zeros((ref.shape[0], spare, LANES), F32)
        ref[:, 0:spare, :] = zeros
        ref[:, ref.shape[1] - spare :, :] = zeros

    sub = lax.broadcasted_iota(jnp.int32, (8, LANES), 0)
    global_row = my_row * rows - PAD + sub * LANES + lane_iota(8)
    latitude = ((global_row.astype(F32) + 0.5) / (rows * n_rows) - 0.5) * math.pi
    on_globe = jnp.logical_and(global_row >= 0, global_row < rows * n_rows)
    cosines = jnp.where(on_globe, jnp.cos(latitude) * 0.125, 0.0)
    for q in range(cosb.shape[0] // LANES):
        row = jnp.broadcast_to(cosines[q : q + 1, :], (LANES, LANES))
        cosb[q * LANES : (q + 1) * LANES, :] = jnp.transpose(row)

    load_words.wait()
    copies_of = LANES // wrd_cols.shape[0]
    for q in range(rows // LANES):
        at = slice(q * LANES, (q + 1) * LANES)
        wrd[at, :] = jnp.transpose(jnp.concatenate([wrd_cols[:, at]] * copies_of, axis=0))

    for copy in load_strips:
        copy.wait()
    packed = rows // 8
    lane = lane_iota(packed)
    for out, tile, shift in ((out_left, 0, 0), (out_right, tiles - 1, HALO)):
        field_part = jnp.zeros((packed, LANES), F32)
        land_part = jnp.zeros((packed, LANES), F32)
        for g in range(8):
            at = slice(g * packed, (g + 1) * packed)
            values = fld[at, tile * LANES : (tile + 1) * LANES]
            land = jnp.where(land_of(wrd[at, :], tile), 1.0, 0.0)
            turn = (HALO * g + shift) % LANES
            if turn:
                values, land = pltpu.roll(values, turn, 1), pltpu.roll(land, turn, 1)
            here = lane // HALO == g
            field_part = jnp.where(here, values, field_part)
            land_part = jnp.where(here, land, land_part)
        out[0:packed, :] = field_part
        out[packed : 2 * packed, :] = land_part
    load_chunk[0].wait()
    if chunks > 1:
        load_chunk[chunks - 1].wait()

    pl.semaphore_wait(barrier, len(peers))

    sends = []

    def send(src, dst, row, col):
        i = len(sends)
        copy = pltpu.make_async_remote_copy(
            src_ref=src, dst_ref=dst, send_sem=send_sem.at[i], recv_sem=recv_sem.at[i],
            device_id=(row, col), device_id_type=MESH,
        )
        copy.start()
        sends.append(copy)

    top, bottom = slice(0, HALO), slice(rows - HALO, rows)
    last_tile = slice(cols - LANES, cols)
    send(out_left, in_right, my_row, left)
    send(out_right, in_left, my_row, right)
    send(fld.at[top, :], fhal.at[HALO : 2 * HALO, :], up, my_col)
    send(fld.at[bottom, :], fhal.at[0:HALO, :], down, my_col)
    send(wrd.at[top, :], whal.at[HALO : 2 * HALO, :], up, my_col)
    send(wrd.at[bottom, :], whal.at[0:HALO, :], down, my_col)
    for column in (left, right):
        pl.semaphore_signal(
            beside_sem, inc=1, device_id=(my_row, column), device_id_type=MESH
        )
    pl.semaphore_signal(far_sem, inc=1, device_id=(far_row, my_col), device_id_type=MESH)

    for c in order[2:]:
        load_chunk[c].wait()

    sets = ((s_num, s_den, r_num, r_den), (s_num2, s_den2, r_num2, r_den2))

    def own_mask(at, which):
        def field_tile(tile):
            return fld[pl.ds(at, ROW_CHUNK), tile * LANES : (tile + 1) * LANES]

        mask_step(
            field_tile, wrd[pl.ds(at, ROW_CHUNK), :], ROW_CHUNK, *sets[which][0:2], tiles
        )

    def own_across(at, which):
        def store(which, tile, value):
            ref = (hn, hd)[which]
            ref[tile, pl.ds(PAD + at, ROW_CHUNK), :] = value

        across_step(ROW_CHUNK, *sets[which], band, tiles, store)

    def own_chunks(first, last):
        own_mask(first * ROW_CHUNK, first % 2)
        for c in range(first, last):
            if c + 1 < last:
                own_mask((c + 1) * ROW_CHUNK, (c + 1) % 2)
            own_across(c * ROW_CHUNK, c % 2)

    own_chunks(0, 3 * chunks // 4)

    pl.semaphore_wait(beside_sem, 2)
    send(fld.at[bottom, last_tile], cornf.at[0 * HALO : 1 * HALO, :], down, right)
    send(fld.at[bottom, 0:LANES], cornf.at[1 * HALO : 2 * HALO, :], down, left)
    send(fld.at[top, last_tile], cornf.at[2 * HALO : 3 * HALO, :], up, right)
    send(fld.at[top, 0:LANES], cornf.at[3 * HALO : 4 * HALO, :], up, left)
    send(wrd.at[bottom, :], cornw.at[0 * HALO : 1 * HALO, :], down, right)
    send(wrd.at[bottom, :], cornw.at[1 * HALO : 2 * HALO, :], down, left)
    send(wrd.at[top, :], cornw.at[2 * HALO : 3 * HALO, :], up, right)
    send(wrd.at[top, :], cornw.at[3 * HALO : 4 * HALO, :], up, left)

    own_chunks(3 * chunks // 4, chunks)

    inside_top, inside_bottom = my_row > 0, my_row < n_rows - 1
    out_rows, out_tiles = rows // 2, tiles // 2

    def finish(num, den):
        value = num / jnp.maximum(den, FLOOR)
        return value, den * value

    zero_sums = (
        jnp.zeros((8, LANES), F32), jnp.zeros((8, LANES), F32), jnp.full((8, LANES), -jnp.inf, F32)
    )

    def gather_sums(sums, value, product, cover):
        return (sums[0] + product, sums[1] + cover, jnp.maximum(sums[2], value))

    def level_one_rows(i0, tile, cosine):
        result = []
        for ref in (hn, hd):
            taps = [ref[tile, pl.ds(PAD + 2 * i0 - 1 + a, 8, stride=2), :] for a in range(4)]
            taps = [t * c for t, c in zip(taps, cosine)]
            result.append((taps[0] + taps[3]) + (taps[1] + taps[2]))
        return result

    def cosine_of(i0):
        taps = [cosb[pl.ds(PAD + 2 * i0 - 1 + a, 8, stride=2), :] for a in range(4)]
        return [taps[0], 3.0 * taps[1], 3.0 * taps[2], taps[3]]

    def level_one_own(i0, which_tiles, sums):
        cosine = cosine_of(i0)
        for tile in which_tiles:
            num, den = level_one_rows(i0, tile, cosine)
            value, product = finish(num, den)
            p1[tile, pl.ds(PAD + i0, 8), :] = product
            d1[tile, pl.ds(PAD + i0, 8), :] = den
            if tile < out_tiles:
                v1[pl.ds(i0, 8), tile * LANES : (tile + 1) * LANES] = value
                sums = gather_sums(sums, value, product, den)
        return sums

    def level_one_inner(which_tiles, sums):
        def pair(c, sums):
            i0 = pl.multiple_of(8 + c * 16, 8)
            sums = level_one_own(i0, which_tiles, sums)
            return level_one_own(i0 + 8, which_tiles, sums)

        return lax.fori_loop(0, out_rows // 16 - 1, pair, sums)

    def level_one_beyond(i0, keep):
        cosine = cosine_of(i0)
        for tile in range(out_tiles + 1):
            num, den = level_one_rows(i0, tile, cosine)
            value, product = finish(num, den)
            p1[tile, PAD + i0 : PAD + i0 + 8, :] = jnp.where(keep, product, 0.0)
            d1[tile, PAD + i0 : PAD + i0 + 8, :] = jnp.where(keep, den, 0.0)

    sums_one = level_one_inner(range(1, out_tiles - 1), zero_sums)

    for copy in sends[0:2]:
        copy.wait()

    def edge_store(at, count, field_value, land_value):
        high, low = pieces(field_value * land_value)
        se_num[at : at + count, 0:LANES] = high
        se_num[at : at + count, LANES : 2 * LANES] = low
        se_den[at : at + count, :] = land_value.astype(BF16)

    def edge_dot(at, count):
        here = slice(at, at + count)
        re_num[here, :] = dot(se_num[here, :], edge[...])
        re_den[here, :] = dot(se_den[here, :], edge[0:128, :])

    def merge_edge(src, dst, count):
        low_half = lane_iota(count) < 64
        for result, ref in ((re_num, hn), (re_den, hd)):
            spill = result[src : src + count, LANES : 2 * LANES]
            here = slice(dst, dst + count)
            last = out_tiles - 1
            ref[0, here, :] = ref[0, here, :] + jnp.where(low_half, spill, 0.0)
            ref[last, here, :] = ref[last, here, :] + jnp.where(low_half, 0.0, spill)
            ref[out_tiles, here, :] = (
                ref[out_tiles, here, :] + result[src : src + count, 0:LANES]
            )

    for g in range(8):
        parts = []
        for base in (0, packed):
            from_right = in_right[base : base + packed, :]
            from_left = in_left[base : base + packed, :]
            turn = (LANES - HALO * g) % LANES
            if turn:
                from_right = pltpu.roll(from_right, turn, 1)
            turn = (LANES - HALO - HALO * g) % LANES
            if turn:
                from_left = pltpu.roll(from_left, turn, 1)
            parts.append(
                jnp.where(
                    lane < HALO, from_right, jnp.where(lane >= LANES - HALO, from_left, 0.0)
                )
            )
        edge_store(g * packed, packed, parts[0], parts[1])
    edge_dot(0, rows)
    merge_edge(0, PAD, rows)
    sums_one = level_one_inner((0, out_tiles - 1, out_tiles), sums_one)

    def inner_groups(ref):
        return [(i0, i0 + 8) for i0 in range(8, ref.shape[0] - 8, 16)]

    def outer_groups(ref, beyond):
        own = [(0, ref.shape[0] - 8)]
        return own + [(-8, ref.shape[0])] if beyond else own

    used = [0, 0]

    def next_level(pin, din, pout, dout, vout):
        out_rows, out_cols = vout.shape
        blocks = out_cols // LANES
        last_level = pout is None
        next_free = list(used)
        used[0] += 2 * blocks * (out_rows + HALO)
        used[1] += 2 * (out_rows + HALO)
        low_half = lane_iota(8) < 64

        def down_rows(ref, i0, tile):
            taps = [ref[tile, pl.ds(PAD + 2 * i0 - 1 + a, 8, stride=2), :] for a in range(4)]
            return 0.125 * (taps[0] + taps[3]) + 0.375 * (taps[1] + taps[2])

        def run(part, sums):
            base, base_e = next_free
            count = 16 * len(part)
            for g, pair in enumerate(part):
                for which, ref in ((0, pin), (1, din)):
                    for tile in range(2 * blocks + 1):
                        value = jnp.concatenate(
                            [down_rows(ref, i0, tile) for i0 in pair], axis=0
                        )
                        high, low = pieces(value)
                        if tile < 2 * blocks:
                            at = base + (which * blocks + tile // 2) * count + 16 * g
                            half = (tile % 2) * LANES
                            sx[at : at + 16, half : half + LANES] = high
                            sx[at : at + 16, 256 + half : 256 + half + LANES] = low
                        else:
                            at = base_e + which * count + 16 * g
                            sxe[at : at + 16, 0:LANES] = high
                            sxe[at : at + 16, LANES : 2 * LANES] = low
            total = 2 * blocks * count
            rx[base : base + total, :] = dot(sx[base : base + total, :], band[...])
            rxe[base_e : base_e + 2 * count, :] = dot(
                sxe[base_e : base_e + 2 * count, :], edge[...]
            )
            starts = [i0 for pair in part for i0 in pair]
            for m, i0 in enumerate(starts):
                beyond = i0 < 0 or i0 >= out_rows
                keep = inside_top if i0 < 0 else inside_bottom
                for tile in range(blocks + (0 if last_level else 1)):
                    both = []
                    for which in range(2):
                        def piece(block, half, which=which):
                            block = block % (blocks + 1)
                            lanes = slice(half * LANES, (half + 1) * LANES)
                            if block == blocks:
                                at = base_e + which * count + 8 * m
                                return rxe[at : at + 8, lanes]
                            at = base + (which * blocks + block) * count + 8 * m
                            return rx[at : at + 8, lanes]

                        both.append(
                            piece(tile, 0)
                            + jnp.where(low_half, piece(tile - 1, 1), piece(tile + 1, 1))
                        )
                    value, product = finish(*both)
                    if beyond:
                        pout[tile, PAD + i0 : PAD + i0 + 8, :] = jnp.where(keep, product, 0.0)
                        dout[tile, PAD + i0 : PAD + i0 + 8, :] = jnp.where(keep, both[1], 0.0)
                        continue
                    if not last_level:
                        pout[tile, PAD + i0 : PAD + i0 + 8, :] = product
                        dout[tile, PAD + i0 : PAD + i0 + 8, :] = both[1]
                    if tile < blocks:
                        vout[i0 : i0 + 8, tile * LANES : (tile + 1) * LANES] = value
                        sums = gather_sums(sums, value, product, both[1])
            next_free[0], next_free[1] = base + total, base_e + 2 * count
            return sums

        return run

    two = next_level(p1, d1, p2, d2, v2)
    three = next_level(p2, d2, p3, d3, v3)
    four = next_level(p3, d3, None, None, v4)
    sums_two, sums_three, sums_four = zero_sums, zero_sums, zero_sums
    groups = inner_groups(v2)
    for i in range(0, len(groups), 4):
        sums_two = two(groups[i : i + 4], sums_two)

    for copy in sends[2:6]:
        copy.wait()

    def halo_store(which, tile, value):
        ref = (hn, hd)[which]
        ref[tile, PAD - HALO : PAD, :] = value[0:HALO, :]
        ref[tile, PAD + rows : PAD + rows + HALO, :] = value[HALO : 2 * HALO, :]

    first_across(
        lambda tile: fhal[:, tile * LANES : (tile + 1) * LANES], whal[...], 2 * HALO,
        s_num, s_den, r_num, r_den, band, tiles, halo_store,
    )
    for copy in sends[6:]:
        copy.wait()
    lane16 = lane_iota(HALO)
    for side in range(2):
        l_at = slice(2 * side * HALO, (2 * side + 1) * HALO)
        r_at = slice((2 * side + 1) * HALO, (2 * side + 2) * HALO)
        is_right, is_left = lane16 < HALO, lane16 >= LANES - HALO
        value = jnp.where(is_right, cornf[r_at, :], jnp.where(is_left, cornf[l_at, :], 0.0))
        land_r = jnp.where(land_of(cornw[r_at, :], 0), 1.0, 0.0)
        land_l = jnp.where(land_of(cornw[l_at, :], tiles - 1), 1.0, 0.0)
        land = jnp.where(is_right, land_r, jnp.where(is_left, land_l, 0.0))
        edge_store(rows + side * HALO, HALO, value, land)
    edge_dot(rows, 2 * HALO)
    merge_edge(rows, PAD - HALO, HALO)
    merge_edge(rows + HALO, PAD + rows, HALO)
    for i0 in (0, out_rows - 8):
        sums_one = level_one_own(i0, range(out_tiles + 1), sums_one)
    level_one_beyond(-8, inside_top)
    level_one_beyond(out_rows, inside_bottom)
    sums_two = two(outer_groups(v2, True), sums_two)
    sums_three = three(inner_groups(v3) + outer_groups(v3, True), sums_three)
    sums_four = four(inner_groups(v4) + outer_groups(v4, False), sums_four)
    all_sums = [sums_one, sums_two, sums_three, sums_four]

    lane = lane_iota(1)
    message = jnp.zeros((1, LANES), F32)

    def whole(x, op):
        return op(op(x, axis=0, keepdims=True), axis=1, keepdims=True)

    for level, sums in enumerate(all_sums):
        for place, (part, op) in enumerate(zip(sums, (jnp.sum, jnp.sum, jnp.max))):
            message = jnp.where(lane == 4 * place + level, whole(part, op), message)

    sent = []

    def exchange(message, buffer, slots, send_sems, recv_sems, index, count, device):
        buffer[...] = message
        slots[index] = message
        copies = []
        for s in range(1, count):
            peer = lax.rem(index + s, count)
            copy = pltpu.make_async_remote_copy(
                src_ref=buffer, dst_ref=slots.at[index],
                send_sem=send_sems.at[s], recv_sem=recv_sems.at[index],
                device_id=device(peer), device_id_type=MESH,
            )
            copy.start()
            copies.append(copy)
        for s in range(1, count):
            peer = lax.rem(index + s, count)
            pltpu.make_async_remote_copy(
                src_ref=buffer, dst_ref=slots.at[peer],
                send_sem=send_sems.at[s], recv_sem=recv_sems.at[peer],
                device_id=device(peer), device_id_type=MESH,
            ).wait_recv()
        added, largest = slots[0], slots[0]
        for i in range(1, count):
            added, largest = added + slots[i], jnp.maximum(largest, slots[i])
        sent.extend(copies)
        return jnp.where(lane < 8, added, largest)

    pl.semaphore_wait(far_sem, 1)
    message = exchange(
        message, msg_b, slot_b, b_send, b_recv, my_row, n_rows, lambda peer: (peer, my_col)
    )
    message = exchange(
        message, msg_a, slot_a, a_send, a_recv, my_col, n_cols, lambda peer: (my_row, peer)
    )
    wide = jnp.broadcast_to(message, (8, LANES))
    covers = pltpu.roll(wide, LANES - 4, 1)
    maxima = pltpu.roll(wide, LANES - 8, 1)
    stats[...] = jnp.where(sub == 0, wide / (covers + EPS), maxima)
    for copy in sent:
        copy.wait_send()


def copy_out(v1, v2, v3, v4, stats):
    def body(*refs):
        ins, outs, small_outs = refs[:5], refs[5:9], refs[9:11]
        small, sem = refs[11:13], refs[13]
        copies = []
        steps = ins[0].shape[0] // 8
        parts = [(0, pl.ds(k * steps, steps)) for k in range(8)]
        parts += [(i, pl.ds(0, ins[i].shape[0])) for i in range(1, 4)]
        for i, at in parts:
            copy = pltpu.make_async_copy(ins[i].at[at, :], outs[i].at[at, :], sem.at[len(copies)])
            copy.start()
            copies.append(copy)
        for which in range(2):
            for i in range(4):
                small[which][i] = ins[4][which, i]
            copy = pltpu.make_async_copy(small[which], small_outs[which], sem.at[len(copies)])
            copy.start()
            copies.append(copy)
        for copy in copies:
            copy.wait()

    shapes = [jax.ShapeDtypeStruct(v.shape, F32) for v in (v1, v2, v3, v4)]
    shapes += [jax.ShapeDtypeStruct((4,), F32)] * 2
    return pl.pallas_call(
        body,
        out_shape=shapes,
        in_specs=[pl.BlockSpec(memory_space=pltpu.VMEM)] * 5,
        out_specs=[pl.BlockSpec(memory_space=pl.ANY)] * 6,
        scratch_shapes=[pltpu.SMEM((4,), F32)] * 2 + [pltpu.SemaphoreType.DMA((13,))],
    )(*[pltpu.with_memory_space_constraint(x, pltpu.VMEM) for x in (v1, v2, v3, v4, stats)])


def per_device(surface_field, land_words):
    rows, cols = surface_field.shape
    n_rows, n_cols = lax.axis_size("rows"), lax.axis_size("cols")
    words = land_words.shape[1]
    chunks = rows // ROW_CHUNK
    blocks = cols // 256
    packed = rows // 8

    def vmem(*shape, dtype=F32):
        return pltpu.VMEM(shape, dtype)

    level = [(rows >> l, cols >> l) for l in range(5)]
    scratch = [
        vmem(rows, cols), vmem(words, rows, dtype=jnp.int32), vmem(rows, LANES, dtype=jnp.int32),
        vmem(2 * HALO, cols), vmem(2 * HALO, LANES, dtype=jnp.int32),
        vmem(2 * packed, LANES), vmem(2 * packed, LANES),
        vmem(2 * packed, LANES), vmem(2 * packed, LANES),
        vmem(4 * HALO, LANES), vmem(4 * HALO, LANES, dtype=jnp.int32),
        vmem(blocks * ROW_CHUNK, 512, dtype=BF16), vmem(blocks * ROW_CHUNK, 256, dtype=BF16),
        vmem(blocks * ROW_CHUNK, 256), vmem(blocks * ROW_CHUNK, 256),
        vmem(blocks * ROW_CHUNK, 512, dtype=BF16), vmem(blocks * ROW_CHUNK, 256, dtype=BF16),
        vmem(blocks * ROW_CHUNK, 256), vmem(blocks * ROW_CHUNK, 256),
        vmem(rows + 2 * HALO, 256, dtype=BF16), vmem(rows + 2 * HALO, LANES, dtype=BF16),
        vmem(rows + 2 * HALO, 256), vmem(rows + 2 * HALO, 256),
        vmem(blocks + 1, rows + 2 * PAD, LANES), vmem(blocks + 1, rows + 2 * PAD, LANES),
        vmem(-(-(rows + 2 * PAD) // LANES) * LANES, LANES),
    ]
    for l in range(1, 4):
        scratch += [vmem(level[l][1] // LANES + 1, level[l][0] + 2 * PAD, LANES)] * 2
    count = sum(level[l][0] + HALO for l in range(2, 5))
    stacked = sum(2 * (level[l][1] // LANES) * (level[l][0] + HALO) for l in range(2, 5))
    scratch += [
        vmem(stacked, 512, dtype=BF16), vmem(2 * count, 256, dtype=BF16),
        vmem(stacked, 256), vmem(2 * count, 256),
        vmem(512, 256, dtype=BF16), vmem(256, 256, dtype=BF16),
        vmem(1, LANES), vmem(1, LANES),
        vmem(n_cols, 1, LANES), vmem(n_rows, 1, LANES),
        pltpu.SemaphoreType.DMA((3 + chunks,)),
        pltpu.SemaphoreType.DMA((14,)), pltpu.SemaphoreType.DMA((14,)),
        pltpu.SemaphoreType.DMA((n_cols,)), pltpu.SemaphoreType.DMA((n_cols,)),
        pltpu.SemaphoreType.DMA((n_rows,)), pltpu.SemaphoreType.DMA((n_rows,)),
        pltpu.SemaphoreType.REGULAR, pltpu.SemaphoreType.REGULAR,
    ]
    out_shape = [pltpu.VMEM(level[l], F32) for l in range(1, 5)]
    out_shape.append(pltpu.VMEM((8, LANES), F32))
    v1, v2, v3, v4, stats = pl.pallas_call(
        kernel,
        out_shape=out_shape,
        in_specs=[pl.BlockSpec(memory_space=pl.ANY)] * 2,
        out_specs=[pl.BlockSpec(memory_space=pltpu.VMEM)] * 5,
        scratch_shapes=scratch,
        compiler_params=pltpu.CompilerParams(
            collective_id=0, has_side_effects=True, vmem_limit_bytes=48 * 1024 * 1024
        ),
    )(
        pltpu.with_memory_space_constraint(surface_field, pltpu.HBM),
        pltpu.with_memory_space_constraint(land_words.T, pltpu.HBM),
    )
    return copy_out(v1, v2, v3, v4, stats)


def solution(mesh):
    spec = P("rows", "cols")
    return jax.shard_map(
        per_device, mesh=mesh, in_specs=(spec, spec),
        out_specs=(spec, spec, spec, spec, P(), P()), check_vma=False,
    )
```
